128 devices in a mesh: rows: 32 (over x, y, core), cores: 4 (over z).
Axes of the slice: x: 4, y: 4, z: 4, core: 2. Of those that a mesh axis runs over, the one named last changes fastest.
Arguments:
- rhs: float32 [524288, 128], P(('rows', 'cores')), may hold values from -6 to 6
- guess: float32 [524288, 128], P(('rows', 'cores')), may hold values from -4 to 4
- degree: float32 [524288], P(('rows', 'cores')), may hold values from 2 to 6
- weights: bfloat16 [4096, 16, 128, 128], P(('rows', 'cores')), may hold values from -0.1875 to 0.1875
- columns: int32 [4096, 16], P(('rows', 'cores')), may hold values from 0 to 287, as said below
- block_counts: int32 [4096], P(('rows', 'cores')), may hold values from 8 to 16, as said below
- send_lists: int32 [128, 128, 2], P(('rows', 'cores')), may hold values from 0 to 31
- aggregates: int32 [524288], P(('rows', 'cores')), may hold values from 0 to 16383
- coarse_diag: float32 [16384], replicated, may hold values from 4 to 32
Outputs:
- smoothed: float32 [524288, 128], P(('rows', 'cores'))
The draws below stay inside these ranges and needn't reach their ends.
Inputs may be any that keep to these rules, and one draw needn't show every extreme that they name: `block_counts`: every block row has 8 or 16 live slots, and the rows of one device have exactly 320 live slots in all. `columns`: on every device, each table index from 32 up is named by at least one live slot.
All inputs are finite; a program needn't handle non-finite values.
Results may differ from the reference program's by a relative error of at most 0.0022.
Values may be sent and summed in bfloat16 or wider, within the bound.
A program may use at most 128 MiB of HBM per device.

```python
import math
import jax
import jax.numpy as jnp
from jax import lax

NB_DEV = 32
BLOCK = 128
SLOTS = 16
MAXB = 2
RHS = 128
NC = 16384
NBLK = 4096
NV = 524288
DEVICES = 128


def counts_table(key):
    base = jax.random.fold_in(key, 11)
    keys = jax.random.split(base, DEVICES)
    perms = jax.vmap(lambda single: jax.random.permutation(single, NB_DEV))(keys)
    hubby = perms < NB_DEV // 4
    return jnp.where(hubby, SLOTS, SLOTS // 2).astype(jnp.int32)


def draw_block_counts(key, part):
    return counts_table(key).reshape(-1)


def draw_columns(key, part):
    counts = counts_table(key)
    live = (jnp.arange(SLOTS, dtype=jnp.int32)[None, None, :] < counts[:, :, None]).reshape(DEVICES, -1).astype(jnp.int32)
    ranks = jnp.cumsum(live, axis=1) - 1
    remote = DEVICES * MAXB
    livecount = NB_DEV * SLOTS * 5 // 8
    keys = jax.random.split(jax.random.fold_in(key, 23), DEVICES)
    perms = jax.vmap(lambda single: jax.random.permutation(single, livecount))(keys).astype(jnp.int32)
    assigned = jnp.take_along_axis(perms, jnp.clip(ranks, 0, livecount - 1), axis=1)
    filler = jax.random.randint(jax.random.fold_in(key, 31), live.shape, 0, NB_DEV + remote)
    chosen = jnp.where((live == 1) & (assigned < remote), NB_DEV + assigned, filler)
    return chosen.reshape(NB_DEV * DEVICES, SLOTS).astype(jnp.int32)


def draw_aggregates(key, part):
    total = NB_DEV * DEVICES * BLOCK
    per_owner = NC // DEVICES
    device = jnp.arange(total, dtype=jnp.int32) // (NB_DEV * BLOCK)
    inside = jax.random.randint(jax.random.fold_in(key, 41), (total,), 0, per_owner)
    anywhere = jax.random.randint(jax.random.fold_in(key, 47), (total,), 0, NC)
    across = jax.random.randint(jax.random.fold_in(key, 43), (total,), 0, 2) == 0
    own = device * per_owner + inside
    return jnp.where(across, anywhere, own).astype(jnp.int32)


def touch_ends(drawn, rng, low, top_value):
    dims = drawn.shape
    index_at = [jax.random.randint(jax.random.fold_in(rng, axis), (), 0, dims[axis]) for axis in range(len(dims))]
    drawn = drawn.at[tuple(index_at)].set(low)
    longest = dims.index(max(dims))
    index_at[longest] = (index_at[longest] + 1) % dims[longest]
    return drawn.at[tuple(index_at)].set(top_value)


def block_levels(rng, shape, shards, least, high):
    def one(axis_at, shards_of):
        steps = jax.random.uniform(jax.random.fold_in(jax.random.fold_in(rng, 6), axis_at), (shards_of,), jnp.float32, least / len(shards), high / len(shards))
        return jnp.repeat(jnp.exp(steps), shape[axis_at] // shards_of).reshape((-1,) + (1,) * (len(shape) - axis_at - 1))

    loudness = one(*shards[0])
    for cut in shards[1:]:
        loudness = loudness * one(*cut)
    return loudness


def bell_draw(own_key, shape, deviation, bound, shards=(), held_as=jnp.bfloat16):
    level = block_levels(own_key, shape, shards, -0.22, 0.18) if shards else 1.0
    drawn = jax.random.normal(own_key, shape, jnp.float32) * deviation * level
    return jnp.minimum(jnp.maximum(drawn, -bound), bound).astype(held_as)


def setup_inputs(seed: int = 0) -> dict:
    key_of = jax.random.split(jax.random.key(seed), 10)
    return {
        "rhs": bell_draw(key_of[0], (NV, RHS), 1.0, 6.0, ((0, 128),), jnp.float32),
        "guess": bell_draw(key_of[1], (NV, RHS), 0.5, 4.0, ((0, 128),), jnp.float32),
        "degree": jnp.clip(jnp.exp(math.log(6.0) - 1.0986123 * jax.random.uniform(key_of[2], (NV,), jnp.float32) ** block_levels(key_of[2], (NV,), ((0, 128),), -0.2, 0.2)), 2.0, 6.0),
        "weights": bell_draw(key_of[3], (NBLK, SLOTS, BLOCK, BLOCK), (BLOCK * 8) ** -0.5, 0.1875, ((0, 128),)),
        "columns": draw_columns(jax.random.fold_in(key_of[9], 71), 0),
        "block_counts": draw_block_counts(jax.random.fold_in(key_of[9], 71), 0),
        "send_lists": touch_ends(jax.random.randint(key_of[6], (DEVICES, DEVICES, MAXB), 0, NB_DEV), jax.random.fold_in(key_of[6], 1), 0, NB_DEV - 1).astype(jnp.int32),
        "aggregates": draw_aggregates(jax.random.fold_in(key_of[9], 71), 0),
        "coarse_diag": jnp.clip(jnp.exp(jax.random.uniform(key_of[8], (NC,), jnp.float32, math.log(4.0), math.log(32.0))), 4.0, 32.0),
    }


damping = 0.7


def reference(rhs, guess, degree, weights, columns, block_counts, send_lists, aggregates, coarse_diag):
    nblk = weights.shape[0]
    live = (jnp.arange(SLOTS, dtype=jnp.int32)[None, :] < block_counts[:, None]).astype(jnp.bfloat16)
    live_weights = weights * live[:, :, None, None]

    def apply(field):
        blocks = field.astype(jnp.bfloat16).reshape(nblk, BLOCK, RHS)

        def one(device):
            local = lax.dynamic_slice_in_dim(blocks, device * NB_DEV, NB_DEV, 0)
            owners = jnp.arange(DEVICES, dtype=jnp.int32)[:, None] * NB_DEV
            wanted = (owners + send_lists[:, device, :]).reshape(-1).astype(jnp.int32)
            table = jnp.concatenate([local, blocks[wanted]], 0)
            wpart = lax.dynamic_slice_in_dim(live_weights, device * NB_DEV, NB_DEV, 0)
            cpart = lax.dynamic_slice_in_dim(columns, device * NB_DEV, NB_DEV, 0)
            return jnp.einsum('bsij,bsjr->bir', wpart.astype(jnp.float32), table[cpart].astype(jnp.float32))

        offsum = lax.map(one, jnp.arange(DEVICES, dtype=jnp.int32)).reshape(-1, RHS)
        return degree[:, None] * field - offsum

    first = guess + damping * (rhs - apply(guess)) / degree[:, None]
    residue = rhs - apply(first)
    coarse = jax.ops.segment_sum(residue, aggregates, num_segments=NC)
    correction = (coarse / coarse_diag[:, None]).astype(jnp.bfloat16)
    second = first + correction[aggregates].astype(jnp.float32)
    return second + damping * (rhs - apply(second)) / degree[:, None]
```

```python
import functools

import jax
import jax.numpy as jnp
from jax import lax
from jax.experimental import pallas as pl
from jax.experimental.pallas import tpu as pltpu
from jax.sharding import PartitionSpec as P

ND = 128
NB = 32
BS = 128
NC = 16384
HALF = NC // 2
TB = NB + 2 * ND
damping = 0.7
MESH = pl.DeviceIdType.MESH
VMEM = pltpu.VMEM
SMEM = pltpu.SMEM
f32 = jnp.float32
bf16 = jnp.bfloat16


def my_place():
    me = lax.axis_index("rows") * 4 + lax.axis_index("cores")
    return me, me // 32, lax.rem(me // 8, 4), lax.rem(me, 4), lax.rem(me // 4, 2)


def place_id(x, y, z, c):
    return ((x * 4 + y) * 2 + c, z)


def peer(k, spot):
    me, x, y, z, c = spot
    m = lax.rem(k * 37, 128)
    px = lax.rem(x + m // 32, 4)
    py = lax.rem(y + lax.rem(m // 8, 4), 4)
    pc = lax.rem(c + lax.rem(m // 4, 2), 2)
    pz = lax.rem(z + lax.rem(m, 4), 4)
    return px, py, pz, pc


def column_of(row):
    return jnp.broadcast_to(row, (BS, BS)).T


def offsum(w_ref, t_ref, col_ref, cnt_ref, b):
    cnt = cnt_ref[b]
    acc = None
    for s in range(0, 16, 2):
        c0 = jnp.where(s < cnt, col_ref[b * 16 + s], TB)
        c1 = jnp.where(s + 1 < cnt, col_ref[b * 16 + s + 1], TB)
        lhs = jnp.concatenate([w_ref[b, s], w_ref[b, s + 1]], axis=1)
        rhs = jnp.concatenate([t_ref[c0], t_ref[c1]], axis=0)
        part = jnp.dot(lhs, rhs, preferred_element_type=f32)
        acc = part if acc is None else acc + part
    return acc


def halo_kernel(
    col_ref, cnt_ref, lst_ref, guess_ref, rhs_ref, deg_ref, agg_ref, w_hbm,
    x1_ref, res_ref, ids_ref,
    w_ref, t1, t2, loc, sbuf, idbuf, wsem, ss, rs, idss, idrs,
):
    spot = my_place()
    me = spot[0]
    wcopy = pltpu.make_async_copy(w_hbm, w_ref, wsem)
    wcopy.start()
    bar = pltpu.get_barrier_semaphore()

    def hello(k, _):
        px, py, pz, pc = peer(k, spot)
        pl.semaphore_signal(bar, inc=1, device_id=place_id(px, py, pz, pc), device_id_type=MESH)
        return 0

    lax.fori_loop(1, ND, hello, 0)

    def cast(b, _):
        v = guess_ref[b].astype(bf16)
        t1[b] = v
        loc[b] = v
        return 0

    lax.fori_loop(0, NB, cast, 0)
    t1[TB] = jnp.zeros((BS, BS), bf16)
    t2[TB] = jnp.zeros((BS, BS), bf16)

    def fill(k):
        px, py, pz, pc = peer(k, spot)
        d = ((px * 4 + py) * 2 + pc) * 4 + pz
        for j in range(2):
            sbuf[k, j] = loc[lst_ref[2 * d + j]]

    def send(k, dst, i):
        px, py, pz, pc = peer(k, spot)
        pltpu.make_async_remote_copy(
            sbuf.at[k], dst.at[pl.ds(NB + 2 * me, 2)], ss.at[i], rs.at[i],
            device_id=place_id(px, py, pz, pc), device_id_type=MESH,
        ).start()

    def fill_ids(k, _):
        px, py, pz, pc = peer(k, spot)
        d = ((px * 4 + py) * 2 + pc) * 4 + pz
        for j in range(2):
            idbuf[k, j] = agg_ref[lst_ref[2 * d + j]]
        return 0

    def send_ids(k, _):
        px, py, pz, pc = peer(k, spot)
        pltpu.make_async_remote_copy(
            idbuf.at[k], ids_ref.at[pl.ds(2 * me, 2)], idss, idrs,
            device_id=place_id(px, py, pz, pc), device_id_type=MESH,
        ).start()
        return 0

    def fill1(k, _):
        fill(k)
        return 0

    lax.fori_loop(1, ND, fill1, 0)
    lax.fori_loop(1, ND, fill_ids, 0)
    for j in range(2):
        own = lst_ref[2 * me + j]
        t1[NB + 2 * me + j] = loc[own]
        ids_ref[2 * me + j] = agg_ref[own]
    pl.semaphore_wait(bar, ND - 1)

    def send1(k, _):
        send(k, t1, 0)
        return 0

    lax.fori_loop(1, ND, send1, 0)
    lax.fori_loop(1, ND, send_ids, 0)
    wcopy.wait()

    def wait_all(i):
        pltpu.make_async_copy(t1.at[pl.ds(0, 254)], t1.at[pl.ds(0, 254)], rs.at[i]).wait()
        pltpu.make_async_copy(t1.at[pl.ds(0, 254)], t1.at[pl.ds(0, 254)], ss.at[i]).wait()

    wait_all(0)

    def first(b, _):
        off = offsum(w_ref, t1, col_ref, cnt_ref, b)
        deg = column_of(deg_ref[b])
        g = guess_ref[b]
        x = g + damping * (rhs_ref[b] - (deg * g - off)) / deg
        x1_ref[b] = x
        v = x.astype(bf16)
        t2[b] = v
        loc[b] = v
        return 0

    lax.fori_loop(0, NB, first, 0)

    def fill2(k, _):
        fill(k)

        @pl.when(k > 2)
        def _():
            send(k - 2, t2, 1)

        return 0

    lax.fori_loop(1, ND, fill2, 0)
    send(ND - 2, t2, 1)
    for j in range(2):
        t2[NB + 2 * me + j] = loc[lst_ref[2 * me + j]]
    send(ND - 1, t2, 1)
    wait_all(1)

    def second(b, _):
        off = offsum(w_ref, t2, col_ref, cnt_ref, b)
        deg = column_of(deg_ref[b])
        res_ref[b] = rhs_ref[b] - (deg * x1_ref[b] - off)
        return 0

    lax.fori_loop(0, NB, second, 0)
    pltpu.make_async_copy(ids_ref.at[pl.ds(0, 254)], ids_ref.at[pl.ds(0, 254)], idrs).wait()
    pltpu.make_async_copy(ids_ref.at[pl.ds(0, 254)], ids_ref.at[pl.ds(0, 254)], idss).wait()


def halo(columns, counts, lists, guess, rhs, degree, agg, weights):
    vm = pl.BlockSpec(memory_space=VMEM)
    sm = pl.BlockSpec(memory_space=SMEM)
    return pl.pallas_call(
        halo_kernel,
        out_shape=(
            jax.ShapeDtypeStruct((NB, BS, BS), f32),
            jax.ShapeDtypeStruct((NB, BS, BS), f32),
            jax.ShapeDtypeStruct((2 * ND, 1, BS), jnp.int32),
        ),
        in_specs=[sm, sm, sm, vm, vm, vm, vm, pl.BlockSpec(memory_space=pl.ANY)],
        out_specs=(vm, vm, vm),
        scratch_shapes=[
            VMEM((NB, 16, BS, BS), bf16),
            VMEM((TB + 1, BS, BS), bf16),
            VMEM((TB + 1, BS, BS), bf16),
            VMEM((NB, BS, BS), bf16),
            VMEM((ND, 2, BS, BS), bf16),
            VMEM((ND, 2, 1, BS), jnp.int32),
            pltpu.SemaphoreType.DMA,
            pltpu.SemaphoreType.DMA((2,)),
            pltpu.SemaphoreType.DMA((2,)),
            pltpu.SemaphoreType.DMA,
            pltpu.SemaphoreType.DMA,
        ],
        compiler_params=pltpu.CompilerParams(
            collective_id=0, has_side_effects=True, vmem_limit_bytes=60 * 2**20
        ),
        name="halo",
    )(columns, counts, lists, guess, rhs, degree, agg, weights)


def scatter_kernel(agg_ref, res_ref, out_ref, b1, b2, b3):
    bufs = (out_ref, b1, b2, b3)
    n = 4096 // 4

    def clear(i, _):
        for buf in bufs:
            for u in range(4):
                buf[pl.ds(i * 32 + u * 8, 8), :] = jnp.zeros((8, BS), f32)
        return 0

    lax.fori_loop(0, NC // 32, clear, 0)

    def add(i, _):
        for u in range(8):
            for q, buf in enumerate(bufs):
                r = q * n + i * 8 + u
                a = agg_ref[r]
                buf[pl.ds(a, 1), :] = buf[pl.ds(a, 1), :] + res_ref[pl.ds(r, 1), :]
        return 0

    lax.fori_loop(0, n // 8, add, 0)

    def total(i, _):
        for u in range(4):
            at = pl.ds(i * 32 + u * 8, 8)
            out_ref[at, :] = (out_ref[at, :] + b1[at, :]) + (b2[at, :] + b3[at, :])
        return 0

    lax.fori_loop(0, NC // 32, total, 0)


def scatter(agg, res):
    vm = pl.BlockSpec(memory_space=VMEM)
    return pl.pallas_call(
        scatter_kernel,
        out_shape=jax.ShapeDtypeStruct((NC, BS), f32),
        in_specs=[pl.BlockSpec(memory_space=SMEM), vm],
        out_specs=vm,
        scratch_shapes=[VMEM((NC, BS), f32)] * 3,
        compiler_params=pltpu.CompilerParams(vmem_limit_bytes=48 * 2**20),
        name="scatter",
    )(agg, res)


UNIT = (48, 48, 32)
BASE = (0, 64 * 48, 128 * 48)


def coarse_kernel(diag_ref, coarse_ref, out_ref, swap, r1, r2, r3, s0, q0, s1, q1, s2, q2, s3, q3, a3s, a3r, a2s, a2r, a1s, a1r, cs, cr):
    me, x, y, z, c = my_place()
    xyz = (x, y, z)
    half = c * HALF
    other = (1 - c) * HALF

    def along(dim, k):
        p = [x, y, z]
        p[dim] = lax.rem(p[dim] + k, 4)
        return place_id(p[0], p[1], p[2], c)

    partner = place_id(x, y, z, 1 - c)
    bar = pltpu.get_barrier_semaphore()
    pl.semaphore_signal(bar, inc=1, device_id=partner, device_id_type=MESH)
    for dim in range(3):
        for k in range(1, 4):
            pl.semaphore_signal(bar, inc=1, device_id=along(dim, k), device_id_type=MESH)
    pl.semaphore_wait(bar, 10)

    def rcopy(src, dst, ssem, rsem, dev):
        return pltpu.make_async_remote_copy(src, dst, ssem, rsem, device_id=dev, device_id_type=MESH)

    def add_into(dst, d0, srcs, rows, step=16):
        def go(i, _):
            v = dst[pl.ds(pl.multiple_of(d0 + i * step, 8), step), :]
            for ref, r0 in srcs:
                v = v + ref[pl.ds(pl.multiple_of(r0 + i * step, 8), step), :]
            dst[pl.ds(pl.multiple_of(d0 + i * step, 8), step), :] = v
            return 0

        lax.fori_loop(0, rows // step, go, 0)

    order = ((0, 1, 2), (1, 2, 0), (2, 0, 1))
    swaps = []
    for k in (1, 2, 3, 0):
        for p in range(3):
            rows = UNIT[p] * 16
            a = lax.rem(xyz[order[p][0]] + k, 4)
            at = BASE[p] + a * rows
            cp = rcopy(
                coarse_ref.at[pl.ds(pl.multiple_of(other + at, 16), rows), :],
                swap.at[pl.ds(pl.multiple_of(at, 16), rows), :],
                s0.at[p, k], q0.at[p, k], partner,
            )
            cp.start()
            swaps.append((k, p, at, rows, cp))
    pend = []
    sent1 = {}
    for k, p, at, rows, cp in swaps:
        cp.wait_recv()
        add_into(swap, at, [(coarse_ref, half + at)], rows)
        if k:
            cp1 = rcopy(
                swap.at[pl.ds(pl.multiple_of(at, 16), rows), :],
                r1.at[k - 1, pl.ds(BASE[p] // 4, rows), :],
                s1.at[p, k - 1], q1.at[p, k - 1], along(order[p][0], k),
            )
            sent1[p, k] = cp1
            pend.append(cp1)
        if len(pend) > 1:
            pend.pop(0).start()
    for cp1 in pend:
        cp1.start()
    cur = []
    for p in range(3):
        rows = UNIT[p] * 16
        at = BASE[p] + xyz[order[p][0]] * rows
        for k in range(1, 4):
            sent1[p, k].wait_recv()
        add_into(swap, at, [(r1.at[k], BASE[p] // 4) for k in range(3)], rows)
        cur.append(at)
    sent2 = {}
    for p in range(3):
        rows = UNIT[p] * 4
        for k in range(1, 4):
            a = lax.rem(xyz[order[p][1]] + k, 4)
            sent2[p, k] = rcopy(
                swap.at[pl.ds(pl.multiple_of(cur[p] + a * rows, 16), rows), :],
                r2.at[k - 1, pl.ds(BASE[p] // 16, rows), :],
                s2.at[p, k - 1], q2.at[p, k - 1], along(order[p][1], k),
            )
            sent2[p, k].start()
    for p in range(3):
        rows = UNIT[p] * 4
        at = cur[p] + xyz[order[p][1]] * rows
        for k in range(1, 4):
            sent2[p, k].wait_recv()
        add_into(swap, at, [(r2.at[k], BASE[p] // 16) for k in range(3)], rows)
        cur[p] = at
    sent3 = {}
    for p in range(3):
        rows = UNIT[p]
        for k in range(1, 4):
            a = lax.rem(xyz[order[p][2]] + k, 4)
            sent3[p, k] = rcopy(
                swap.at[pl.ds(pl.multiple_of(cur[p] + a * rows, 16), rows), :],
                r3.at[k - 1, pl.ds(BASE[p] // 64, rows), :],
                s3.at[p, k - 1], q3.at[p, k - 1], along(order[p][2], k),
            )
            sent3[p, k].start()
    for p in range(3):
        rows = UNIT[p]
        at = cur[p] + xyz[order[p][2]] * rows
        for k in range(1, 4):
            sent3[p, k].wait_recv()
        cur[p] = at
        for i in range(rows // 16):
            v = swap[pl.ds(pl.multiple_of(at + i * 16, 8), 16), :]
            for k in range(3):
                v = v + r3[k, pl.ds(BASE[p] // 64 + i * 16, 16), :]
            div = jnp.concatenate(
                [jnp.full((1, BS), diag_ref[half + at + i * 16 + r], f32) for r in range(16)], axis=0
            )
            out_ref[pl.ds(pl.multiple_of(half + at + i * 16, 16), 16), :] = (v / div).astype(bf16)
    sends = list(sent1.values()) + list(sent2.values()) + list(sent3.values()) + [s[4] for s in swaps]

    def spread(sent, p, dim, at, rows, ssem, rsem):
        for k in range(1, 4):
            ref = out_ref.at[pl.ds(pl.multiple_of(half + at, 16), rows), :]
            cp = rcopy(ref, ref, ssem.at[p, k - 1], rsem.at[p, k - 1], along(dim, k))
            cp.start()
            sent[p, k] = cp
            sends.append(cp)

    g3, g2, g1 = {}, {}, {}
    for p in range(3):
        spread(g3, p, order[p][2], cur[p], UNIT[p], a3s, a3r)
    for p in range(3):
        for k in range(1, 4):
            g3[p, k].wait_recv()
        at = cur[p] - xyz[order[p][2]] * UNIT[p]
        cur[p] = at
        spread(g2, p, order[p][1], at, UNIT[p] * 4, a2s, a2r)
    swapped = []

    def hand_over(p, a, k):
        rows = UNIT[p] * 16
        ref = out_ref.at[pl.ds(pl.multiple_of(half + BASE[p] + a * rows, 16), rows), :]
        cp = rcopy(ref, ref, cs.at[p, k], cr.at[p, k], partner)
        cp.start()
        sends.append(cp)
        swapped.append(cp)

    for p in range(3):
        for k in range(1, 4):
            g2[p, k].wait_recv()
        at = cur[p] - xyz[order[p][1]] * UNIT[p] * 4
        cur[p] = at
        spread(g1, p, order[p][0], at, UNIT[p] * 16, a1s, a1r)
        hand_over(p, xyz[order[p][0]], 0)
    for k in range(1, 4):
        for p in range(3):
            g1[p, k].wait_recv()
            hand_over(p, lax.rem(xyz[order[p][0]] + 4 - k, 4), k)
    for cp in swapped:
        cp.wait_recv()
    for cp in sends:
        cp.wait_send()


def coarse_solve(diag, coarse):
    vm = pl.BlockSpec(memory_space=VMEM)
    dma = pltpu.SemaphoreType.DMA
    return pl.pallas_call(
        coarse_kernel,
        out_shape=jax.ShapeDtypeStruct((NC, BS), bf16),
        in_specs=[pl.BlockSpec(memory_space=SMEM), vm],
        out_specs=vm,
        scratch_shapes=[
            VMEM((HALF, BS), f32),
            VMEM((3, HALF // 4, BS), f32),
            VMEM((3, HALF // 16, BS), f32),
            VMEM((3, HALF // 64, BS), f32),
            dma((3, 4)), dma((3, 4)),
            dma((3, 3)), dma((3, 3)), dma((3, 3)), dma((3, 3)), dma((3, 3)), dma((3, 3)),
            dma((3, 3)), dma((3, 3)), dma((3, 3)), dma((3, 3)), dma((3, 3)), dma((3, 3)),
            dma((3, 4)), dma((3, 4)),
        ],
        compiler_params=pltpu.CompilerParams(
            collective_id=1, has_side_effects=True, vmem_limit_bytes=40 * 2**20
        ),
        name="coarse",
    )(diag, coarse)


def final_kernel(
    col_ref, cnt_ref, agg_ref, ids_ref, corr_ref, x1_ref, res_ref, deg_ref, w_hbm,
    out_ref, w_ref, cf, table, pcl, tile, wsem,
):
    wcopy = pltpu.make_async_copy(w_hbm, w_ref, wsem)
    wcopy.start()

    def widen(i, _):
        for u in range(4):
            at = pl.ds(pl.multiple_of(i * 64 + u * 16, 16), 16)
            cf[at, :] = corr_ref[at, :].astype(f32)
        return 0

    lax.fori_loop(0, NC // 64, widen, 0)
    table[TB] = jnp.zeros((BS, BS), bf16)

    def local(b, _):
        for r in range(BS):
            pcl[b, pl.ds(r, 1), :] = cf[pl.ds(agg_ref[b * BS + r], 1), :]
        table[b] = pcl[b].astype(bf16)
        return 0

    lax.fori_loop(0, NB, local, 0)

    def remote(t, _):
        for r in range(BS):
            tile[pl.ds(r, 1), :] = cf[pl.ds(ids_ref[t * BS + r], 1), :]
        table[NB + t] = tile[...].astype(bf16)
        return 0

    lax.fori_loop(0, 2 * ND, remote, 0)
    wcopy.wait()

    def final(b, _):
        off = offsum(w_ref, table, col_ref, cnt_ref, b)
        deg = column_of(deg_ref[b])
        pc = pcl[b]
        out_ref[b] = (x1_ref[b] + pc) + damping * (res_ref[b] - (deg * pc - off)) / deg
        return 0

    lax.fori_loop(0, NB, final, 0)


def final(columns, counts, agg, ids, corr, x1, res, degree, weights):
    vm = pl.BlockSpec(memory_space=VMEM)
    sm = pl.BlockSpec(memory_space=SMEM)
    return pl.pallas_call(
        final_kernel,
        out_shape=jax.ShapeDtypeStruct((NB, BS, BS), f32),
        in_specs=[sm, sm, sm, sm, vm, vm, vm, vm, pl.BlockSpec(memory_space=pl.ANY)],
        out_specs=vm,
        scratch_shapes=[
            VMEM((NB, 16, BS, BS), bf16),
            VMEM((NC, BS), f32),
            VMEM((TB + 1, BS, BS), bf16),
            VMEM((NB, BS, BS), f32),
            VMEM((BS, BS), f32),
            pltpu.SemaphoreType.DMA,
        ],
        compiler_params=pltpu.CompilerParams(vmem_limit_bytes=60 * 2**20),
        name="final",
    )(columns, counts, agg, ids, corr, x1, res, degree, weights)


def body(rhs, guess, degree, weights, columns, block_counts, send_lists, aggregates, coarse_diag):
    cols = columns.reshape(-1)
    lists = send_lists.reshape(-1)
    deg = degree.reshape(NB, 1, BS)
    x1, res, ids = halo(
        cols, block_counts, lists,
        guess.reshape(NB, BS, BS), rhs.reshape(NB, BS, BS), deg,
        aggregates.reshape(NB, 1, BS), weights,
    )
    coarse = scatter(aggregates, res.reshape(NB * BS, BS))
    corr = coarse_solve(coarse_diag, coarse)
    out = final(cols, block_counts, aggregates, ids.reshape(-1), corr, x1, res, deg, weights)
    return out.reshape(NB * BS, BS)


def solution(mesh):
    both = ("rows", "cores")
    return jax.shard_map(
        body,
        mesh=mesh,
        in_specs=(
            P(both, None),
            P(both, None),
            P(both),
            P(both, None, None, None),
            P(both, None),
            P(both),
            P(both, None, None),
            P(both),
            P(),
        ),
        out_specs=P(both, None),
        check_vma=False,
    )
```

```python
import functools

import jax
import jax.numpy as jnp
from jax import lax
from jax.experimental import pallas as pl
from jax.experimental.pallas import tpu as pltpu
from jax.sharding import PartitionSpec as P

ND = 128
NB = 32
BS = 128
NC = 16384
HALF = NC // 2
TB = NB + 2 * ND
HUBS = 8
damping = 0.7
MESH = pl.DeviceIdType.MESH
VMEM = pltpu.VMEM
SMEM = pltpu.SMEM
f32 = jnp.float32
bf16 = jnp.bfloat16


def my_place():
    me = lax.axis_index("rows") * 4 + lax.axis_index("cores")
    return me, me // 32, lax.rem(me // 8, 4), lax.rem(me, 4), lax.rem(me // 4, 2)


def place_id(x, y, z, c):
    return ((x * 4 + y) * 2 + c, z)


def peer(k, spot):
    me, x, y, z, c = spot
    m = lax.rem(k * 37, 128)
    px = lax.rem(x + m // 32, 4)
    py = lax.rem(y + lax.rem(m // 8, 4), 4)
    pc = lax.rem(c + lax.rem(m // 4, 2), 2)
    pz = lax.rem(z + lax.rem(m, 4), 4)
    return px, py, pz, pc


def column_of(row):
    return jnp.broadcast_to(row, (BS, BS)).T


def find_hubs(cnt_ref, hub_ref, rank_ref):
    seen = jnp.int32(0)
    at = [jnp.int32(0)] * HUBS
    for b in range(NB):
        rank_ref[b] = seen
        seen = seen + jnp.where(cnt_ref[b] > 8, 1, 0)
        for k in range(HUBS):
            at[k] = at[k] + jnp.where(seen <= k, 1, 0)
    for k in range(HUBS):
        hub_ref[k] = jnp.minimum(at[k], NB - 1)


def half_row(w_ref, t_ref, col_ref, b, s0):
    acc = None
    for s in range(s0, s0 + 8, 2):
        lhs = jnp.concatenate([w_ref[b, s], w_ref[b, s + 1]], axis=1)
        rhs = jnp.concatenate([t_ref[col_ref[s, b]], t_ref[col_ref[s + 1, b]]], axis=0)
        part = jnp.dot(lhs, rhs, preferred_element_type=f32)
        acc = part if acc is None else acc + part
    return acc


def stencil(w_ref, t_ref, col_ref, cnt_ref, hub_ref, rank_ref, hacc, finish, width=4):
    def hubs(i, _):
        for u in range(width):
            k = i * width + u
            hacc[k] = half_row(w_ref, t_ref, col_ref, hub_ref[k], 8)
        return 0

    lax.fori_loop(0, HUBS // width, hubs, 0)

    def rows(i, _):
        for u in range(width):
            b = i * width + u
            extra = hacc[jnp.minimum(rank_ref[b], HUBS - 1)]
            off = half_row(w_ref, t_ref, col_ref, b, 0)
            off = off + jnp.where(cnt_ref[b] > 8, extra, 0.0)
            finish(b, off)
        return 0

    lax.fori_loop(0, NB // width, rows, 0)


def halo_kernel(
    col_ref, cnt_ref, lst_ref, guess_ref, rhs_ref, deg_ref, agg_ref, w_hbm,
    x1_ref, res_ref, ids_ref,
    w_ref, t1, t2, loc, sbuf, idbuf, hacc, hub_ref, rank_ref, wsem, ss, rs, idss, idrs,
):
    spot = my_place()
    me = spot[0]
    wcopy = pltpu.make_async_copy(w_hbm, w_ref, wsem)
    wcopy.start()
    bar = pltpu.get_barrier_semaphore()

    def cast(b, _):
        v = guess_ref[b].astype(bf16)
        t1[b] = v
        loc[b] = v
        return 0

    lax.fori_loop(0, NB, cast, 0)

    def prepare(k, _):
        px, py, pz, pc = peer(k, spot)
        row = (px * 4 + py) * 2 + pc
        d = row * 4 + pz
        pl.semaphore_signal(bar, inc=1, device_id=(row, pz), device_id_type=MESH)
        for j in range(2):
            own = lst_ref[j, d]
            sbuf[k, j] = loc[own]
            idbuf[k, j] = agg_ref[own]
        return 0

    lax.fori_loop(1, ND, prepare, 0)
    for j in range(2):
        own = lst_ref[j, me]
        t1[NB + 2 * me + j] = loc[own]
        ids_ref[2 * me + j] = agg_ref[own]
    pl.semaphore_wait(bar, ND - 1)

    def send(k, dst, i, dev):
        pltpu.make_async_remote_copy(
            sbuf.at[k], dst.at[pl.ds(NB + 2 * me, 2)], ss.at[i], rs.at[i],
            device_id=dev, device_id_type=MESH,
        ).start()

    def send1(k, _):
        px, py, pz, pc = peer(k, spot)
        dev = place_id(px, py, pz, pc)
        pltpu.make_async_remote_copy(
            idbuf.at[k], ids_ref.at[pl.ds(2 * me, 2)], idss, idrs,
            device_id=dev, device_id_type=MESH,
        ).start()
        send(k, t1, 0, dev)
        return 0

    lax.fori_loop(1, ND, send1, 0)
    find_hubs(cnt_ref, hub_ref, rank_ref)
    wcopy.wait()

    def wait_all(i):
        pltpu.make_async_copy(t1.at[pl.ds(0, 254)], t1.at[pl.ds(0, 254)], rs.at[i]).wait()
        pltpu.make_async_copy(t1.at[pl.ds(0, 254)], t1.at[pl.ds(0, 254)], ss.at[i]).wait()

    wait_all(0)

    def first(b, off):
        deg = column_of(deg_ref[b])
        g = guess_ref[b]
        x = g + damping * (rhs_ref[b] - (deg * g - off)) / deg
        x1_ref[b] = x
        v = x.astype(bf16)
        t2[b] = v
        loc[b] = v

    stencil(w_ref, t1, col_ref, cnt_ref, hub_ref, rank_ref, hacc, first)

    def fill2(k, _):
        px, py, pz, pc = peer(k, spot)
        d = ((px * 4 + py) * 2 + pc) * 4 + pz
        for j in range(2):
            sbuf[k, j] = loc[lst_ref[j, d]]

        @pl.when(k > 2)
        def _():
            send(k - 2, t2, 1, place_id(*peer(k - 2, spot)))

        return 0

    lax.fori_loop(1, ND, fill2, 0)
    send(ND - 2, t2, 1, place_id(*peer(ND - 2, spot)))
    for j in range(2):
        t2[NB + 2 * me + j] = loc[lst_ref[j, me]]
    send(ND - 1, t2, 1, place_id(*peer(ND - 1, spot)))
    wait_all(1)

    def second(b, off):
        deg = column_of(deg_ref[b])
        res_ref[b] = rhs_ref[b] - (deg * x1_ref[b] - off)

    stencil(w_ref, t2, col_ref, cnt_ref, hub_ref, rank_ref, hacc, second)
    pltpu.make_async_copy(ids_ref.at[pl.ds(0, 254)], ids_ref.at[pl.ds(0, 254)], idrs).wait()
    pltpu.make_async_copy(ids_ref.at[pl.ds(0, 254)], ids_ref.at[pl.ds(0, 254)], idss).wait()


def halo(columns, counts, lists, guess, rhs, degree, agg, weights):
    vm = pl.BlockSpec(memory_space=VMEM)
    sm = pl.BlockSpec(memory_space=SMEM)
    return pl.pallas_call(
        halo_kernel,
        out_shape=(
            jax.ShapeDtypeStruct((NB, BS, BS), f32),
            jax.ShapeDtypeStruct((NB, BS, BS), f32),
            jax.ShapeDtypeStruct((2 * ND, 1, BS), jnp.int32),
        ),
        in_specs=[sm, sm, sm, vm, vm, vm, vm, pl.BlockSpec(memory_space=pl.ANY)],
        out_specs=(vm, vm, vm),
        scratch_shapes=[
            VMEM((NB, 16, BS, BS), bf16),
            VMEM((TB, BS, BS), bf16),
            VMEM((TB, BS, BS), bf16),
            VMEM((NB, BS, BS), bf16),
            VMEM((ND, 2, BS, BS), bf16),
            VMEM((ND, 2, 1, BS), jnp.int32),
            VMEM((HUBS, BS, BS), f32),
            SMEM((HUBS,), jnp.int32),
            SMEM((NB,), jnp.int32),
            pltpu.SemaphoreType.DMA,
            pltpu.SemaphoreType.DMA((2,)),
            pltpu.SemaphoreType.DMA((2,)),
            pltpu.SemaphoreType.DMA,
            pltpu.SemaphoreType.DMA,
        ],
        compiler_params=pltpu.CompilerParams(
            collective_id=0, has_side_effects=True, vmem_limit_bytes=60 * 2**20
        ),
        name="halo",
    )(columns, counts, lists, guess, rhs, degree, agg, weights)


def scatter_kernel(agg_ref, res_hbm, out_hbm, b0, b1, b2, b3, res_ref, rsem, osem):
    bufs = (b0, b1, b2, b3)
    n = 4096 // 4
    rcopy = pltpu.make_async_copy(res_hbm, res_ref, rsem)
    rcopy.start()

    def clear(i, _):
        for buf in bufs:
            for u in range(8):
                buf[pl.ds(i * 64 + u * 8, 8), :] = jnp.zeros((8, BS), f32)
        return 0

    lax.fori_loop(0, NC // 64, clear, 0)
    rcopy.wait()

    def add(i, _):
        for u in range(8):
            for q, buf in enumerate(bufs):
                r = q * n + i * 8 + u
                a = agg_ref[r]
                buf[pl.ds(a, 1), :] = buf[pl.ds(a, 1), :] + res_ref[pl.ds(r, 1), :]
        return 0

    lax.fori_loop(0, n // 8, add, 0)
    chunk = NC // 8
    outs = []
    for c in range(8):

        def total(i, _):
            for u in range(8):
                at = pl.ds(c * chunk + i * 64 + u * 8, 8)
                b0[at, :] = (b0[at, :] + b1[at, :]) + (b2[at, :] + b3[at, :])
            return 0

        lax.fori_loop(0, chunk // 64, total, 0)
        part = pl.ds(c * chunk, chunk)
        cp = pltpu.make_async_copy(b0.at[part, :], out_hbm.at[part, :], osem.at[c])
        outs.append(cp)
        if c:
            outs[c - 1].start()
    outs[-1].start()
    for cp in outs:
        cp.wait()


def scatter(agg, res):
    hbm = pl.BlockSpec(memory_space=pltpu.HBM)
    return pl.pallas_call(
        scatter_kernel,
        out_shape=jax.ShapeDtypeStruct((NC, BS), f32),
        in_specs=[pl.BlockSpec(memory_space=SMEM), hbm],
        out_specs=hbm,
        scratch_shapes=[VMEM((NC, BS), f32)] * 4
        + [VMEM((NB * BS, BS), f32), pltpu.SemaphoreType.DMA, pltpu.SemaphoreType.DMA((8,))],
        compiler_params=pltpu.CompilerParams(vmem_limit_bytes=63 * 2**20),
        name="scatter",
    )(agg, res)


UNIT = (48, 48, 32)
BASE = (0, 64 * 48, 128 * 48)


def coarse_kernel(
    col_ref, cnt_ref, diag_ref, deg_ref, agg_hbm, ids_hbm, coarse_hbm, x1_hbm, res_hbm, w_hbm,
    out_ref,
    w_ref, x1_ref, res_ref, agg_ref, ids_ref, acc, swap, r1, r2, r3, corr, cf, table, pcl, tile0, tile1,
    hacc, hub_ref, rank_ref, lsem, hsem, s0, q0, s1, q1, s2, q2, s3, q3,
    a3s, a3r, a2s, a2r, a1s, a1r, cs, cr,
):
    me, x, y, z, c = my_place()
    xyz = (x, y, z)
    half = c * HALF
    other = (1 - c) * HALF

    def along(dim, k):
        p = [x, y, z]
        p[dim] = lax.rem(p[dim] + k, 4)
        return place_id(p[0], p[1], p[2], c)

    partner = place_id(x, y, z, 1 - c)
    bar = pltpu.get_barrier_semaphore()
    pl.semaphore_signal(bar, inc=1, device_id=partner, device_id_type=MESH)
    for dim in range(3):
        for k in range(1, 4):
            pl.semaphore_signal(bar, inc=1, device_id=along(dim, k), device_id_type=MESH)

    def rcopy(src, dst, ssem, rsem, dev):
        return pltpu.make_async_remote_copy(src, dst, ssem, rsem, device_id=dev, device_id_type=MESH)

    def rows_at(at, rows):
        return pl.ds(pl.multiple_of(at, 16), rows)

    def add_into(dst, d0, srcs, rows, step=32):
        if rows % step:
            step = 16

        def go(i, _):
            v = dst[rows_at(d0 + i * step, step), :]
            for ref, r0 in srcs:
                v = v + ref[rows_at(r0 + i * step, step), :]
            dst[rows_at(d0 + i * step, step), :] = v
            return 0

        lax.fori_loop(0, rows // step, go, 0)

    order = ((0, 1, 2), (1, 2, 0), (2, 0, 1))
    pieces = []
    for k in (1, 2, 3, 0):
        for p in range(3):
            rows = UNIT[p] * 16
            at = BASE[p] + lax.rem(xyz[order[p][0]] + k, 4) * rows
            hcopy = pltpu.make_async_copy(
                coarse_hbm.at[rows_at(half + at, rows), :], acc.at[rows_at(at, rows), :], hsem.at[p, k]
            )
            hcopy.start()
            pieces.append((k, p, at, rows, hcopy))
    pl.semaphore_wait(bar, 10)
    sends = []
    swaps = []
    for k, p, at, rows, hcopy in pieces:
        cp = rcopy(
            coarse_hbm.at[rows_at(other + at, rows), :], swap.at[rows_at(at, rows), :],
            s0.at[p, k], q0.at[p, k], partner,
        )
        cp.start()
        swaps.append(cp)
    loads = [
        pltpu.make_async_copy(src, dst, lsem.at[i])
        for i, (src, dst) in enumerate(
            ((w_hbm, w_ref), (x1_hbm, x1_ref), (res_hbm, res_ref), (agg_hbm, agg_ref), (ids_hbm, ids_ref))
        )
    ]
    pend = []
    sent1 = {}
    for (k, p, at, rows, hcopy), cp in zip(pieces, swaps):
        hcopy.wait()
        cp.wait_recv()
        add_into(acc, at, [(swap, at)], rows)
        if k:
            cp1 = rcopy(
                acc.at[rows_at(at, rows), :], r1.at[k - 1, pl.ds(BASE[p] // 4, rows), :],
                s1.at[p, k - 1], q1.at[p, k - 1], along(order[p][0], k),
            )
            sent1[p, k] = cp1
            pend.append(cp1)
        if len(pend) > 1:
            pend.pop(0).start()
    for cp1 in pend:
        cp1.start()
    for cp in loads:
        cp.start()
    find_hubs(cnt_ref, hub_ref, rank_ref)
    cur = []
    sent2 = {}
    for p in (2, 0, 1):
        rows = UNIT[p] * 16
        at = BASE[p] + xyz[order[p][0]] * rows
        for k in range(1, 4):
            sent1[p, k].wait_recv()
        add_into(acc, at, [(r1.at[k], BASE[p] // 4) for k in range(3)], rows)
        n2 = UNIT[p] * 4
        for k in range(1, 4):
            a = lax.rem(xyz[order[p][1]] + k, 4)
            sent2[p, k] = rcopy(
                acc.at[rows_at(at + a * n2, n2), :], r2.at[k - 1, pl.ds(BASE[p] // 16, n2), :],
                s2.at[p, k - 1], q2.at[p, k - 1], along(order[p][1], k),
            )
            sent2[p, k].start()
        cur.append((p, at + xyz[order[p][1]] * n2))
    sent3 = {}
    last = []
    for p, at in cur:
        rows = UNIT[p] * 4
        for k in range(1, 4):
            sent2[p, k].wait_recv()
        add_into(acc, at, [(r2.at[k], BASE[p] // 16) for k in range(3)], rows)
        n3 = UNIT[p]
        for k in range(1, 4):
            a = lax.rem(xyz[order[p][2]] + k, 4)
            sent3[p, k] = rcopy(
                acc.at[rows_at(at + a * n3, n3), :], r3.at[k - 1, pl.ds(BASE[p] // 64, n3), :],
                s3.at[p, k - 1], q3.at[p, k - 1], along(order[p][2], k),
            )
            sent3[p, k].start()
        last.append((p, at + xyz[order[p][2]] * n3))

    def spread(sent, p, dim, at, rows, ssem, rsem):
        for k in range(1, 4):
            ref = corr.at[rows_at(half + at, rows), :]
            cp = rcopy(ref, ref, ssem.at[p, k - 1], rsem.at[p, k - 1], along(dim, k))
            cp.start()
            sent[p, k] = cp
            sends.append(cp)

    def widen(at, rows):
        def go(i, _):
            here = rows_at(at + i * 16, 16)
            cf[here, :] = corr[here, :].astype(f32)
            return 0

        lax.fori_loop(0, rows // 16, go, 0)

    g3, g2, g1 = {}, {}, {}
    for p, at in last:
        rows = UNIT[p]
        for k in range(1, 4):
            sent3[p, k].wait_recv()
        for i in range(rows // 16):
            v = acc[rows_at(at + i * 16, 16), :]
            for k in range(3):
                v = v + r3[k, pl.ds(BASE[p] // 64 + i * 16, 16), :]
            div = jnp.concatenate(
                [jnp.full((1, BS), diag_ref[half + at + i * 16 + r], f32) for r in range(16)], axis=0
            )
            corr[rows_at(half + at + i * 16, 16), :] = (v / div).astype(bf16)
        spread(g3, p, order[p][2], at, rows, a3s, a3r)
    cur = []
    for p, at in last:
        for k in range(1, 4):
            g3[p, k].wait_recv()
        at = at - xyz[order[p][2]] * UNIT[p]
        cur.append((p, at))
        spread(g2, p, order[p][1], at, UNIT[p] * 4, a2s, a2r)
    swapped = []

    def hand_over(p, a, k):
        rows = UNIT[p] * 16
        ref = corr.at[rows_at(half + BASE[p] + a * rows, rows), :]
        cp = rcopy(ref, ref, cs.at[p, k], cr.at[p, k], partner)
        cp.start()
        sends.append(cp)
        swapped.append((cp, other + BASE[p] + a * rows, rows))
        widen(half + BASE[p] + a * rows, rows)

    for p, at in cur:
        for k in range(1, 4):
            g2[p, k].wait_recv()
        at = at - xyz[order[p][1]] * UNIT[p] * 4
        spread(g1, p, order[p][0], at, UNIT[p] * 16, a1s, a1r)
        hand_over(p, xyz[order[p][0]], 0)
    for k in (1, 3, 2):
        for p in (2, 0, 1):
            g1[p, k].wait_recv()
            hand_over(p, lax.rem(xyz[order[p][0]] + 4 - k, 4), k)
    for cp, at, rows in swapped:
        cp.wait_recv()
        widen(at, rows)
    for cp in loads:
        cp.wait()

    def local(b, _):
        for r in range(BS):
            pcl[b, pl.ds(r, 1), :] = cf[pl.ds(agg_ref[b * BS + r], 1), :]

        @pl.when(b > 0)
        def _():
            table[b - 1] = pcl[b - 1].astype(bf16)

        return 0

    lax.fori_loop(0, NB, local, 0)
    table[NB - 1] = pcl[NB - 1].astype(bf16)

    def pick(t, tile):
        for r in range(BS):
            tile[pl.ds(r, 1), :] = cf[pl.ds(ids_ref[t * BS + r], 1), :]

    pick(0, tile0)

    def remote(i, _):
        t = 2 * i
        pick(t + 1, tile1)
        table[NB + t] = tile0[...].astype(bf16)
        pick(t + 2, tile0)
        table[NB + t + 1] = tile1[...].astype(bf16)
        return 0

    lax.fori_loop(0, ND - 1, remote, 0)
    pick(2 * ND - 1, tile1)
    table[TB - 2] = tile0[...].astype(bf16)
    table[TB - 1] = tile1[...].astype(bf16)

    def third(b, off):
        deg = column_of(deg_ref[b])
        pc = pcl[b]
        out_ref[b] = (x1_ref[b] + pc) + damping * (res_ref[b] - (deg * pc - off)) / deg

    stencil(w_ref, table, col_ref, cnt_ref, hub_ref, rank_ref, hacc, third)
    for cp in list(sent1.values()) + list(sent2.values()) + list(sent3.values()) + swaps + sends:
        cp.wait_send()


def coarse_leg(columns, counts, diag, degree, agg, ids, coarse, x1, res, weights):
    vm = pl.BlockSpec(memory_space=VMEM)
    sm = pl.BlockSpec(memory_space=SMEM)
    hbm = pl.BlockSpec(memory_space=pltpu.HBM)
    dma = pltpu.SemaphoreType.DMA
    return pl.pallas_call(
        coarse_kernel,
        out_shape=jax.ShapeDtypeStruct((NB, BS, BS), f32),
        in_specs=[sm, sm, sm, vm, hbm, hbm, hbm, hbm, hbm, hbm],
        out_specs=vm,
        scratch_shapes=[
            VMEM((NB, 16, BS, BS), bf16),
            VMEM((NB, BS, BS), f32),
            VMEM((NB, BS, BS), f32),
            SMEM((NB * BS,), jnp.int32),
            SMEM((2 * ND * BS,), jnp.int32),
            VMEM((HALF, BS), f32),
            VMEM((HALF, BS), f32),
            VMEM((3, HALF // 4, BS), f32),
            VMEM((3, HALF // 16, BS), f32),
            VMEM((3, HALF // 64, BS), f32),
            VMEM((NC, BS), bf16),
            VMEM((NC, BS), f32),
            VMEM((TB, BS, BS), bf16),
            VMEM((NB, BS, BS), f32),
            VMEM((BS, BS), f32),
            VMEM((BS, BS), f32),
            VMEM((HUBS, BS, BS), f32),
            SMEM((HUBS,), jnp.int32),
            SMEM((NB,), jnp.int32),
            dma((5,)),
            dma((3, 4)), dma((3, 4)), dma((3, 4)),
            dma((3, 3)), dma((3, 3)), dma((3, 3)), dma((3, 3)), dma((3, 3)), dma((3, 3)),
            dma((3, 3)), dma((3, 3)), dma((3, 3)), dma((3, 3)), dma((3, 3)), dma((3, 3)),
            dma((3, 4)), dma((3, 4)),
        ],
        compiler_params=pltpu.CompilerParams(
            collective_id=1, has_side_effects=True, vmem_limit_bytes=63 * 2**20
        ),
        name="coarse_leg",
    )(columns, counts, diag, degree, agg, ids, coarse, x1, res, weights)


def body(rhs, guess, degree, weights, columns, block_counts, send_lists, aggregates, coarse_diag):
    cols = columns.T
    lists = send_lists[0].T
    deg = degree.reshape(NB, 1, BS)
    x1, res, ids = halo(
        cols, block_counts, lists,
        guess.reshape(NB, BS, BS), rhs.reshape(NB, BS, BS), deg,
        aggregates.reshape(NB, 1, BS), weights,
    )
    coarse = scatter(aggregates, res.reshape(NB * BS, BS))
    out = coarse_leg(
        cols, block_counts, coarse_diag, deg, aggregates, ids.reshape(-1), coarse, x1, res, weights
    )
    return out.reshape(NB * BS, BS)


def solution(mesh):
    both = ("rows", "cores")
    return jax.shard_map(
        body,
        mesh=mesh,
        in_specs=(
            P(both, None),
            P(both, None),
            P(both),
            P(both, None, None, None),
            P(both, None),
            P(both),
            P(both, None, None),
            P(both),
            P(),
        ),
        out_specs=P(both, None),
        check_vma=False,
    )
```

```python
import functools

import jax
import jax.numpy as jnp
from jax import lax
from jax.experimental import pallas as pl
from jax.experimental.pallas import tpu as pltpu
from jax.sharding import PartitionSpec as P

ND = 128
NB = 32
BS = 128
NC = 16384
HALF = NC // 2
TB = NB + 2 * ND
GROUP = 8
HUBS = 8
damping = 0.7
MESH = pl.DeviceIdType.MESH
VMEM = pltpu.VMEM
SMEM = pltpu.SMEM
f32 = jnp.float32
bf16 = jnp.bfloat16


def my_place():
    me = lax.axis_index("rows") * 4 + lax.axis_index("cores")
    return me, me // 32, lax.rem(me // 8, 4), lax.rem(me, 4), lax.rem(me // 4, 2)


def place_id(x, y, z, c):
    return ((x * 4 + y) * 2 + c, z)


def peer(k, spot):
    me, x, y, z, c = spot
    m = lax.rem(k * 19, 128)
    px = lax.rem(x + m // 32, 4)
    py = lax.rem(y + lax.rem(m // 8, 4), 4)
    pc = lax.rem(c + lax.rem(m // 4, 2), 2)
    pz = lax.rem(z + lax.rem(m, 4), 4)
    return px, py, pz, pc


def column_of(row):
    return jnp.broadcast_to(row, (BS, BS)).T


def find_hubs(cnt_ref, hub_ref, rank_ref):
    seen = jnp.int32(0)
    at = [jnp.int32(0)] * HUBS
    for b in range(NB):
        rank_ref[b] = seen
        seen = seen + jnp.where(cnt_ref[b] > 8, 1, 0)
        for k in range(HUBS):
            at[k] = at[k] + jnp.where(seen <= k, 1, 0)
    for k in range(HUBS):
        hub_ref[k] = jnp.minimum(at[k], NB - 1)


def half_row(w_ref, t_ref, col_ref, b, s0):
    acc = None
    for s in range(s0, s0 + 8, 2):
        lhs = jnp.concatenate([w_ref[b, s], w_ref[b, s + 1]], axis=1)
        rhs = jnp.concatenate([t_ref[col_ref[s, b]], t_ref[col_ref[s + 1, b]]], axis=0)
        part = jnp.dot(lhs, rhs, preferred_element_type=f32)
        acc = part if acc is None else acc + part
    return acc


def stencil(w_ref, t_ref, col_ref, cnt_ref, hub_ref, rank_ref, hacc, finish, width=4):
    def hubs(i, _):
        for u in range(width):
            k = i * width + u
            hacc[k] = half_row(w_ref, t_ref, col_ref, hub_ref[k], 8)
        return 0

    lax.fori_loop(0, HUBS // width, hubs, 0)

    def rows(i, _):
        for u in range(width):
            b = i * width + u
            extra = hacc[jnp.minimum(rank_ref[b], HUBS - 1)]
            off = half_row(w_ref, t_ref, col_ref, b, 0)
            off = off + jnp.where(cnt_ref[b] > 8, extra, 0.0)
            finish(b, off)
        return 0

    lax.fori_loop(0, NB // width, rows, 0)


def halo_kernel(
    col_ref, cnt_ref, lst_ref, guess_ref, rhs_ref, deg_ref, agg_ref, w_hbm,
    x1_ref, res_ref, ids_ref,
    w_ref, t1, t2, loc, sbuf, idbuf, hacc, hub_ref, rank_ref, wsem, ss, rs, idss, idrs,
):
    spot = my_place()
    me = spot[0]
    wcopy = pltpu.make_async_copy(w_hbm, w_ref, wsem)
    wcopy.start()
    bar = pltpu.get_barrier_semaphore()

    def hello(k, _):
        d = lax.rem(me + k, ND)
        pl.semaphore_signal(bar, inc=1, device_id=(d // 4, lax.rem(d, 4)), device_id_type=MESH)
        return 0

    lax.fori_loop(1, ND, hello, 0)

    def cast(b, _):
        v = guess_ref[b].astype(bf16)
        t1[b] = v
        loc[b] = v
        return 0

    lax.fori_loop(0, NB, cast, 0)

    def prepare(k, _):
        px, py, pz, pc = peer(k, spot)
        row = (px * 4 + py) * 2 + pc
        d = row * 4 + pz
        for j in range(2):
            own = lst_ref[j, d]
            sbuf[k, j] = loc[own]
            idbuf[k, j] = agg_ref[own]
        return 0

    lax.fori_loop(1, ND, prepare, 0)
    for j in range(2):
        own = lst_ref[j, me]
        t1[NB + 2 * me + j] = loc[own]
        ids_ref[2 * me + j] = agg_ref[own]
    pl.semaphore_wait(bar, ND - 1)

    def send(k, dst, i, dev):
        pltpu.make_async_remote_copy(
            sbuf.at[k], dst.at[pl.ds(NB + 2 * me, 2)], ss.at[i], rs.at[i],
            device_id=dev, device_id_type=MESH,
        ).start()

    def send1(k, _):
        px, py, pz, pc = peer(k, spot)
        dev = place_id(px, py, pz, pc)
        pltpu.make_async_remote_copy(
            idbuf.at[k], ids_ref.at[pl.ds(2 * me, 2)], idss, idrs,
            device_id=dev, device_id_type=MESH,
        ).start()
        send(k, t1, 0, dev)
        return 0

    lax.fori_loop(1, ND, send1, 0)
    find_hubs(cnt_ref, hub_ref, rank_ref)
    wcopy.wait()

    def wait_all(i):
        pltpu.make_async_copy(t1.at[pl.ds(0, 254)], t1.at[pl.ds(0, 254)], rs.at[i]).wait()
        pltpu.make_async_copy(t1.at[pl.ds(0, 254)], t1.at[pl.ds(0, 254)], ss.at[i]).wait()

    wait_all(0)

    def first(b, off):
        deg = column_of(deg_ref[b])
        g = guess_ref[b]
        x = g + damping * (rhs_ref[b] - (deg * g - off)) / deg
        x1_ref[b] = x
        v = x.astype(bf16)
        t2[b] = v
        loc[b] = v

    stencil(w_ref, t1, col_ref, cnt_ref, hub_ref, rank_ref, hacc, first)

    def fill2(k, _):
        px, py, pz, pc = peer(k, spot)
        d = ((px * 4 + py) * 2 + pc) * 4 + pz
        for j in range(2):
            sbuf[k, j] = loc[lst_ref[j, d]]

        @pl.when(k > 2)
        def _():
            send(k - 2, t2, 1, place_id(*peer(k - 2, spot)))

        return 0

    lax.fori_loop(1, ND, fill2, 0)
    send(ND - 2, t2, 1, place_id(*peer(ND - 2, spot)))
    for j in range(2):
        t2[NB + 2 * me + j] = loc[lst_ref[j, me]]
    send(ND - 1, t2, 1, place_id(*peer(ND - 1, spot)))
    wait_all(1)

    def second(b, off):
        deg = column_of(deg_ref[b])
        res_ref[b] = rhs_ref[b] - (deg * x1_ref[b] - off)

    stencil(w_ref, t2, col_ref, cnt_ref, hub_ref, rank_ref, hacc, second)
    pltpu.make_async_copy(ids_ref.at[pl.ds(0, 254)], ids_ref.at[pl.ds(0, 254)], idrs).wait()
    pltpu.make_async_copy(ids_ref.at[pl.ds(0, 254)], ids_ref.at[pl.ds(0, 254)], idss).wait()


def halo(columns, counts, lists, guess, rhs, degree, agg, weights):
    vm = pl.BlockSpec(memory_space=VMEM)
    sm = pl.BlockSpec(memory_space=SMEM)
    return pl.pallas_call(
        halo_kernel,
        out_shape=(
            jax.ShapeDtypeStruct((NB, BS, BS), f32),
            jax.ShapeDtypeStruct((NB, BS, BS), f32),
            jax.ShapeDtypeStruct((2 * ND, 1, BS), jnp.int32),
        ),
        in_specs=[sm, sm, sm, vm, vm, vm, vm, pl.BlockSpec(memory_space=pl.ANY)],
        out_specs=(vm, vm, vm),
        scratch_shapes=[
            VMEM((NB, 16, BS, BS), bf16),
            VMEM((TB, BS, BS), bf16),
            VMEM((TB, BS, BS), bf16),
            VMEM((NB, BS, BS), bf16),
            VMEM((ND, 2, BS, BS), bf16),
            VMEM((ND, 2, 1, BS), jnp.int32),
            VMEM((HUBS, BS, BS), f32),
            SMEM((HUBS,), jnp.int32),
            SMEM((NB,), jnp.int32),
            pltpu.SemaphoreType.DMA,
            pltpu.SemaphoreType.DMA((2,)),
            pltpu.SemaphoreType.DMA((2,)),
            pltpu.SemaphoreType.DMA,
            pltpu.SemaphoreType.DMA,
        ],
        compiler_params=pltpu.CompilerParams(
            collective_id=0, has_side_effects=True, vmem_limit_bytes=60 * 2**20
        ),
        name="halo",
    )(columns, counts, lists, guess, rhs, degree, agg, weights)


def scatter_kernel(agg_ref, res_hbm, out_hbm, b0, b1, b2, b3, res_ref, rsem, osem):
    bufs = (b0, b1, b2, b3)
    n = 4096 // 4
    rcopy = pltpu.make_async_copy(res_hbm, res_ref, rsem)
    rcopy.start()

    def clear(i, _):
        for buf in bufs:
            for u in range(8):
                buf[pl.ds(i * 64 + u * 8, 8), :] = jnp.zeros((8, BS), f32)
        return 0

    lax.fori_loop(0, NC // 64, clear, 0)
    rcopy.wait()

    def add(i, _):
        for u in range(8):
            for q, buf in enumerate(bufs):
                r = q * n + i * 8 + u
                a = agg_ref[r]
                buf[pl.ds(a, 1), :] = buf[pl.ds(a, 1), :] + res_ref[pl.ds(r, 1), :]
        return 0

    lax.fori_loop(0, n // 8, add, 0)
    chunk = NC // 8
    outs = []
    for c in range(8):

        def total(i, _):
            for u in range(8):
                at = pl.ds(c * chunk + i * 64 + u * 8, 8)
                b0[at, :] = (b0[at, :] + b1[at, :]) + (b2[at, :] + b3[at, :])
            return 0

        lax.fori_loop(0, chunk // 64, total, 0)
        part = pl.ds(c * chunk, chunk)
        cp = pltpu.make_async_copy(b0.at[part, :], out_hbm.at[part, :], osem.at[c])
        outs.append(cp)
        if c:
            outs[c - 1].start()
    outs[-1].start()
    for cp in outs:
        cp.wait()


def scatter(agg, res):
    hbm = pl.BlockSpec(memory_space=pltpu.HBM)
    return pl.pallas_call(
        scatter_kernel,
        out_shape=jax.ShapeDtypeStruct((NC, BS), f32),
        in_specs=[pl.BlockSpec(memory_space=SMEM), hbm],
        out_specs=hbm,
        scratch_shapes=[VMEM((NC, BS), f32)] * 4
        + [VMEM((NB * BS, BS), f32), pltpu.SemaphoreType.DMA, pltpu.SemaphoreType.DMA((8,))],
        compiler_params=pltpu.CompilerParams(vmem_limit_bytes=63 * 2**20),
        name="scatter",
    )(agg, res)


UNIT = (48, 48, 32)
BASE = (0, 64 * 48, 128 * 48)


def coarse_kernel(
    col_ref, cnt_ref, diag_ref, deg_ref, agg_hbm, ids_hbm, coarse_hbm, x1_hbm, res_hbm, w_hbm,
    out_ref,
    w_ref, x1_ref, res_ref, id0, id1, id2, id3, acc, swap, sb1, r1, r2, r3, corr, cf, table, pcl, tile0, tile1,
    hacc, hub_ref, rank_ref, lsem, isem, hsem, s0, q0, s1, q1, s2, q2, s3, q3,
    a3s, a3r, a2s, a2r, a1s, a1r, cs, cr,
):
    me, x, y, z, c = my_place()
    xyz = (x, y, z)
    half = c * HALF
    other = (1 - c) * HALF

    def along(dim, k):
        p = [x, y, z]
        p[dim] = lax.rem(p[dim] + k, 4)
        return place_id(p[0], p[1], p[2], c)

    partner = place_id(x, y, z, 1 - c)
    bar = pltpu.get_barrier_semaphore()
    pl.semaphore_signal(bar, inc=1, device_id=partner, device_id_type=MESH)
    for dim in range(3):
        for k in range(1, 4):
            pl.semaphore_signal(bar, inc=1, device_id=along(dim, k), device_id_type=MESH)

    def rcopy(src, dst, ssem, rsem, dev):
        return pltpu.make_async_remote_copy(src, dst, ssem, rsem, device_id=dev, device_id_type=MESH)

    def rows_at(at, rows):
        return pl.ds(pl.multiple_of(at, 16), rows)

    def add_into(dst, d0, srcs, rows, step=32):
        if rows % step:
            step = 16

        def go(i, _):
            v = dst[rows_at(d0 + i * step, step), :]
            for ref, r0 in srcs:
                v = v + ref[rows_at(r0 + i * step, step), :].astype(f32)
            dst[rows_at(d0 + i * step, step), :] = v
            return 0

        lax.fori_loop(0, rows // step, go, 0)

    def pack_sum(dst, d0, at, rows):
        def go(i, _):
            here = rows_at(at + i * 16, 16)
            dst[rows_at(d0 + i * 16, 16), :] = (acc[here, :] + swap[here, :]).astype(bf16)
            return 0

        lax.fori_loop(0, rows // 16, go, 0)

    order = ((0, 1, 2), (1, 2, 0), (2, 0, 1))
    pieces = []
    for k in (1, 2, 3, 0):
        for p in range(3):
            rows = UNIT[p] * 16
            at = BASE[p] + lax.rem(xyz[order[p][0]] + k, 4) * rows
            hcopy = pltpu.make_async_copy(
                coarse_hbm.at[rows_at(half + at, rows), :], acc.at[rows_at(at, rows), :], hsem.at[p, k]
            )
            hcopy.start()
            pieces.append((k, p, at, rows, hcopy))
    pl.semaphore_wait(bar, 10)
    sends = []
    swaps = []
    for k, p, at, rows, hcopy in pieces:
        cp = rcopy(
            coarse_hbm.at[rows_at(other + at, rows), :], swap.at[rows_at(at, rows), :],
            s0.at[p, k], q0.at[p, k], partner,
        )
        cp.start()
        swaps.append(cp)
    loads = [
        pltpu.make_async_copy(src, dst, lsem.at[i])
        for i, (src, dst) in enumerate(
            ((w_hbm, w_ref), (x1_hbm, x1_ref), (res_hbm, res_ref))
        )
    ]
    pend = []
    sent1 = {}
    for (k, p, at, rows, hcopy), cp in zip(pieces, swaps):
        hcopy.wait()
        cp.wait_recv()
        if k == 0:
            add_into(acc, at, [(swap, at)], rows)
        else:
            pack_sum(sb1.at[k - 1], BASE[p] // 4, at, rows)
            cp1 = rcopy(
                sb1.at[k - 1, pl.ds(BASE[p] // 4, rows), :], r1.at[k - 1, pl.ds(BASE[p] // 4, rows), :],
                s1.at[p, k - 1], q1.at[p, k - 1], along(order[p][0], k),
            )
            sent1[p, k] = cp1
            pend.append(cp1)
        if len(pend) > 1:
            pend.pop(0).start()
    for cp1 in pend:
        cp1.start()
    for cp in loads:
        cp.start()
    find_hubs(cnt_ref, hub_ref, rank_ref)
    id_refs = (id0, id1, id2, id3)

    def fetch(src, n, g):
        part = src.at[pl.ds(pl.multiple_of(n * GROUP * BS, GROUP * BS), GROUP * BS)]
        return pltpu.make_async_copy(part, id_refs[g], isem.at[g])

    for g in range(2):
        fetch(agg_hbm, g, g).start()
        fetch(ids_hbm, g + 2, g + 2).start()
    cur = []
    sent2 = {}
    for p in (2, 0, 1):
        rows = UNIT[p] * 16
        at = BASE[p] + xyz[order[p][0]] * rows
        for k in range(1, 4):
            sent1[p, k].wait_recv()
        add_into(acc, at, [(r1.at[k], BASE[p] // 4) for k in range(3)], rows)
        n2 = UNIT[p] * 4
        for k in range(1, 4):
            a = lax.rem(xyz[order[p][1]] + k, 4)
            sent2[p, k] = rcopy(
                acc.at[rows_at(at + a * n2, n2), :], r2.at[k - 1, pl.ds(BASE[p] // 16, n2), :],
                s2.at[p, k - 1], q2.at[p, k - 1], along(order[p][1], k),
            )
            sent2[p, k].start()
        cur.append((p, at + xyz[order[p][1]] * n2))
    sent3 = {}
    last = []
    for p, at in cur:
        rows = UNIT[p] * 4
        for k in range(1, 4):
            sent2[p, k].wait_recv()
        add_into(acc, at, [(r2.at[k], BASE[p] // 16) for k in range(3)], rows)
        n3 = UNIT[p]
        for k in range(1, 4):
            a = lax.rem(xyz[order[p][2]] + k, 4)
            sent3[p, k] = rcopy(
                acc.at[rows_at(at + a * n3, n3), :], r3.at[k - 1, pl.ds(BASE[p] // 64, n3), :],
                s3.at[p, k - 1], q3.at[p, k - 1], along(order[p][2], k),
            )
            sent3[p, k].start()
        last.append((p, at + xyz[order[p][2]] * n3))

    def spread(sent, p, dim, at, rows, ssem, rsem):
        for k in range(1, 4):
            ref = corr.at[rows_at(half + at, rows), :]
            cp = rcopy(ref, ref, ssem.at[p, k - 1], rsem.at[p, k - 1], along(dim, k))
            cp.start()
            sent[p, k] = cp
            sends.append(cp)

    def widen(at, rows):
        def go(i, _):
            here = rows_at(at + i * 16, 16)
            cf[here, :] = corr[here, :].astype(f32)
            return 0

        lax.fori_loop(0, rows // 16, go, 0)

    g3, g2, g1 = {}, {}, {}
    for p, at in last:
        rows = UNIT[p]
        for k in range(1, 4):
            sent3[p, k].wait_recv()
        for i in range(rows // 16):
            v = acc[rows_at(at + i * 16, 16), :]
            for k in range(3):
                v = v + r3[k, pl.ds(BASE[p] // 64 + i * 16, 16), :]
            div = jnp.concatenate(
                [jnp.full((1, BS), diag_ref[half + at + i * 16 + r], f32) for r in range(16)], axis=0
            )
            corr[rows_at(half + at + i * 16, 16), :] = (v / div).astype(bf16)
        spread(g3, p, order[p][2], at, rows, a3s, a3r)
    cur = []
    for p, at in last:
        for k in range(1, 4):
            g3[p, k].wait_recv()
        at = at - xyz[order[p][2]] * UNIT[p]
        cur.append((p, at))
        spread(g2, p, order[p][1], at, UNIT[p] * 4, a2s, a2r)
    swapped = []

    def hand_over(p, a, k):
        rows = UNIT[p] * 16
        ref = corr.at[rows_at(half + BASE[p] + a * rows, rows), :]
        cp = rcopy(ref, ref, cs.at[p, k], cr.at[p, k], partner)
        cp.start()
        sends.append(cp)
        swapped.append((cp, other + BASE[p] + a * rows, rows))
        widen(half + BASE[p] + a * rows, rows)

    for p, at in cur:
        for k in range(1, 4):
            g2[p, k].wait_recv()
        at = at - xyz[order[p][1]] * UNIT[p] * 4
        spread(g1, p, order[p][0], at, UNIT[p] * 16, a1s, a1r)
        hand_over(p, xyz[order[p][0]], 0)
    for k in (1, 3, 2):
        for p in (2, 0, 1):
            g1[p, k].wait_recv()
            hand_over(p, lax.rem(xyz[order[p][0]] + 4 - k, 4), k)
    for cp, at, rows in swapped:
        cp.wait_recv()
        widen(at, rows)
    for cp in loads:
        cp.wait()

    def local(i, _):
        for g in range(2):
            n = 2 * i + g
            fetch(agg_hbm, n, g).wait()
            for u in range(GROUP):
                b = n * GROUP + u
                for r in range(BS):
                    pcl[b, pl.ds(r, 1), :] = cf[pl.ds(id_refs[g][u * BS + r], 1), :]
                if u:
                    table[b - 1] = pcl[b - 1].astype(bf16)
            table[b] = pcl[b].astype(bf16)

            @pl.when(i == 0)
            def _():
                fetch(agg_hbm, n + 2, g).start()

        return 0

    lax.fori_loop(0, 2, local, 0)
    for g in range(2):
        fetch(ids_hbm, g, g).start()
    tiles = (tile0, tile1)

    def remote(i, _):
        for g in range(4):
            n = 4 * i + g
            fetch(ids_hbm, n, g).wait()
            for u in range(GROUP):
                t = NB + n * GROUP + u
                tile = tiles[u % 2]
                for r in range(BS):
                    tile[pl.ds(r, 1), :] = cf[pl.ds(id_refs[g][u * BS + r], 1), :]
                if u:
                    table[t - 1] = tiles[(u - 1) % 2][...].astype(bf16)
            table[t] = tile[...].astype(bf16)

            @pl.when(i < 2 * ND // GROUP // 4 - 1)
            def _():
                fetch(ids_hbm, n + 4, g).start()

        return 0

    lax.fori_loop(0, 2 * ND // GROUP // 4, remote, 0)

    def third(b, off):
        deg = column_of(deg_ref[b])
        pc = pcl[b]
        out_ref[b] = (x1_ref[b] + pc) + damping * (res_ref[b] - (deg * pc - off)) / deg

    stencil(w_ref, table, col_ref, cnt_ref, hub_ref, rank_ref, hacc, third)
    for cp in list(sent1.values()) + list(sent2.values()) + list(sent3.values()) + swaps + sends:
        cp.wait_send()


def coarse_leg(columns, counts, diag, degree, agg, ids, coarse, x1, res, weights):
    vm = pl.BlockSpec(memory_space=VMEM)
    sm = pl.BlockSpec(memory_space=SMEM)
    hbm = pl.BlockSpec(memory_space=pltpu.HBM)
    dma = pltpu.SemaphoreType.DMA
    return pl.pallas_call(
        coarse_kernel,
        out_shape=jax.ShapeDtypeStruct((NB, BS, BS), f32),
        in_specs=[sm, sm, sm, vm, hbm, hbm, hbm, hbm, hbm, hbm],
        out_specs=vm,
        scratch_shapes=[
            VMEM((NB, 16, BS, BS), bf16),
            VMEM((NB, BS, BS), f32),
            VMEM((NB, BS, BS), f32),
            SMEM((GROUP * BS,), jnp.int32),
            SMEM((GROUP * BS,), jnp.int32),
            SMEM((GROUP * BS,), jnp.int32),
            SMEM((GROUP * BS,), jnp.int32),
            VMEM((HALF, BS), f32),
            VMEM((HALF, BS), f32),
            VMEM((3, HALF // 4, BS), bf16),
            VMEM((3, HALF // 4, BS), bf16),
            VMEM((3, HALF // 16, BS), f32),
            VMEM((3, HALF // 64, BS), f32),
            VMEM((NC, BS), bf16),
            VMEM((NC, BS), f32),
            VMEM((TB, BS, BS), bf16),
            VMEM((NB, BS, BS), f32),
            VMEM((BS, BS), f32),
            VMEM((BS, BS), f32),
            VMEM((HUBS, BS, BS), f32),
            SMEM((HUBS,), jnp.int32),
            SMEM((NB,), jnp.int32),
            dma((3,)), dma((4,)),
            dma((3, 4)), dma((3, 4)), dma((3, 4)),
            dma((3, 3)), dma((3, 3)), dma((3, 3)), dma((3, 3)), dma((3, 3)), dma((3, 3)),
            dma((3, 3)), dma((3, 3)), dma((3, 3)), dma((3, 3)), dma((3, 3)), dma((3, 3)),
            dma((3, 4)), dma((3, 4)),
        ],
        compiler_params=pltpu.CompilerParams(
            collective_id=1, has_side_effects=True, vmem_limit_bytes=63 * 2**20
        ),
        name="coarse_leg",
    )(columns, counts, diag, degree, agg, ids, coarse, x1, res, weights)


def body(rhs, guess, degree, weights, columns, block_counts, send_lists, aggregates, coarse_diag):
    cols = columns.T
    lists = send_lists[0].T
    deg = degree.reshape(NB, 1, BS)
    x1, res, ids = halo(
        cols, block_counts, lists,
        guess.reshape(NB, BS, BS), rhs.reshape(NB, BS, BS), deg,
        aggregates.reshape(NB, 1, BS), weights,
    )
    coarse = scatter(aggregates, res.reshape(NB * BS, BS))
    out = coarse_leg(
        cols, block_counts, coarse_diag, deg, aggregates, ids.reshape(-1), coarse, x1, res, weights
    )
    return out.reshape(NB * BS, BS)


def solution(mesh):
    both = ("rows", "cores")
    return jax.shard_map(
        body,
        mesh=mesh,
        in_specs=(
            P(both, None),
            P(both, None),
            P(both),
            P(both, None, None, None),
            P(both, None),
            P(both),
            P(both, None, None),
            P(both),
            P(),
        ),
        out_specs=P(both, None),
        check_vma=False,
    )
```

```python
import functools

import jax
import jax.numpy as jnp
from jax import lax
from jax.experimental import pallas as pl
from jax.experimental.pallas import tpu as pltpu
from jax.sharding import PartitionSpec as P

ND = 128
NB = 32
BS = 128
NC = 16384
HALF = NC // 2
TB = NB + 2 * ND
GROUP = 8
HUBS = 8
damping = 0.7
MESH = pl.DeviceIdType.MESH
VMEM = pltpu.VMEM
SMEM = pltpu.SMEM
f32 = jnp.float32
bf16 = jnp.bfloat16


def my_place():
    me = lax.axis_index("rows") * 4 + lax.axis_index("cores")
    return me, me // 32, lax.rem(me // 8, 4), lax.rem(me, 4), lax.rem(me // 4, 2)


def place_id(x, y, z, c):
    return ((x * 4 + y) * 2 + c, z)


def peer(k, spot):
    me, x, y, z, c = spot
    m = lax.rem(k * 19, 128)
    px = lax.rem(x + m // 32, 4)
    py = lax.rem(y + lax.rem(m // 8, 4), 4)
    pc = lax.rem(c + lax.rem(m // 4, 2), 2)
    pz = lax.rem(z + lax.rem(m, 4), 4)
    return px, py, pz, pc


def column_of(row):
    return jnp.broadcast_to(row, (BS, BS)).T


def find_hubs(cnt_ref, hub_ref, rank_ref):
    seen = jnp.int32(0)
    at = [jnp.int32(0)] * HUBS
    for b in range(NB):
        rank_ref[b] = seen
        seen = seen + jnp.where(cnt_ref[b] > 8, 1, 0)
        for k in range(HUBS):
            at[k] = at[k] + jnp.where(seen <= k, 1, 0)
    for k in range(HUBS):
        hub_ref[k] = jnp.minimum(at[k], NB - 1)


def half_row(w_ref, t_ref, col_ref, b, s0):
    acc = None
    for s in range(s0, s0 + 8, 2):
        lhs = jnp.concatenate([w_ref[b, s], w_ref[b, s + 1]], axis=1)
        rhs = jnp.concatenate([t_ref[col_ref[s, b]], t_ref[col_ref[s + 1, b]]], axis=0)
        part = jnp.dot(lhs, rhs, preferred_element_type=f32)
        acc = part if acc is None else acc + part
    return acc


def stencil(w_ref, t_ref, col_ref, cnt_ref, hub_ref, rank_ref, hacc, finish, width=4):
    def hubs(i, _):
        for u in range(width):
            k = i * width + u
            hacc[k] = half_row(w_ref, t_ref, col_ref, hub_ref[k], 8)
        return 0

    lax.fori_loop(0, HUBS // width, hubs, 0)

    def rows(i, _):
        for u in range(width):
            b = i * width + u
            extra = hacc[jnp.minimum(rank_ref[b], HUBS - 1)]
            off = half_row(w_ref, t_ref, col_ref, b, 0)
            off = off + jnp.where(cnt_ref[b] > 8, extra, 0.0)
            finish(b, off)
        return 0

    lax.fori_loop(0, NB // width, rows, 0)


def halo_kernel(
    col_ref, cnt_ref, lst_ref, guess_hbm, rhs_hbm, deg_ref, agg_ref, w_hbm,
    x1_ref, res_ref, ids_ref,
    w_ref, guess_ref, rhs_ref, t1, t2, loc, sbuf, idbuf, hacc, hub_ref, rank_ref, lsem, ss, rs, idss, idrs,
):
    spot = my_place()
    me = spot[0]
    bar = pltpu.get_barrier_semaphore()

    def hello(k, _):
        d = lax.rem(me + k, ND)
        pl.semaphore_signal(bar, inc=1, device_id=(d // 4, lax.rem(d, 4)), device_id_type=MESH)
        return 0

    gcopy = pltpu.make_async_copy(guess_hbm, guess_ref, lsem.at[0])
    gcopy.start()
    lax.fori_loop(1, ND, hello, 0)
    gcopy.wait()
    loads = [
        pltpu.make_async_copy(rhs_hbm, rhs_ref, lsem.at[1]),
        pltpu.make_async_copy(w_hbm, w_ref, lsem.at[2]),
    ]

    def cast(b, _):
        v = guess_ref[b].astype(bf16)
        t1[b] = v
        loc[b] = v
        return 0

    lax.fori_loop(0, NB, cast, 0)
    pl.semaphore_wait(bar, ND - 1)

    def send(k, dst, i):
        pltpu.make_async_remote_copy(
            sbuf.at[k], dst.at[pl.ds(NB + 2 * me, 2)], ss.at[i], rs.at[i],
            device_id=place_id(*peer(k, spot)), device_id_type=MESH,
        ).start()

    def send_field(dst, i):
        def fill(k, _):
            px, py, pz, pc = peer(k, spot)
            d = ((px * 4 + py) * 2 + pc) * 4 + pz
            for j in range(2):
                sbuf[k, j] = loc[lst_ref[j, d]]

            @pl.when(k > 2)
            def _():
                send(k - 2, dst, i)

            return 0

        lax.fori_loop(1, ND, fill, 0)
        send(ND - 2, dst, i)
        for j in range(2):
            dst[NB + 2 * me + j] = loc[lst_ref[j, me]]
        send(ND - 1, dst, i)

    send_field(t1, 0)
    for cp in loads:
        cp.start()

    def send_ids(k, _):
        px, py, pz, pc = peer(k, spot)
        row = (px * 4 + py) * 2 + pc
        for j in range(2):
            idbuf[k, j] = agg_ref[lst_ref[j, row * 4 + pz]]

        @pl.when(k > 1)
        def _():
            ship_ids(k - 1)

        return 0

    def ship_ids(k):
        pltpu.make_async_remote_copy(
            idbuf.at[k], ids_ref.at[pl.ds(2 * me, 2)], idss, idrs,
            device_id=place_id(*peer(k, spot)), device_id_type=MESH,
        ).start()

    lax.fori_loop(1, ND, send_ids, 0)
    for j in range(2):
        ids_ref[2 * me + j] = agg_ref[lst_ref[j, me]]
    ship_ids(ND - 1)
    find_hubs(cnt_ref, hub_ref, rank_ref)
    for cp in loads:
        cp.wait()

    def wait_all(i):
        pltpu.make_async_copy(t1.at[pl.ds(0, 254)], t1.at[pl.ds(0, 254)], rs.at[i]).wait()
        pltpu.make_async_copy(t1.at[pl.ds(0, 254)], t1.at[pl.ds(0, 254)], ss.at[i]).wait()

    wait_all(0)

    def first(b, off):
        deg = column_of(deg_ref[b])
        g = guess_ref[b]
        x = g + damping * (rhs_ref[b] - (deg * g - off)) / deg
        x1_ref[b] = x
        v = x.astype(bf16)
        t2[b] = v
        loc[b] = v

    stencil(w_ref, t1, col_ref, cnt_ref, hub_ref, rank_ref, hacc, first)

    send_field(t2, 1)
    wait_all(1)

    def second(b, off):
        deg = column_of(deg_ref[b])
        res_ref[b] = rhs_ref[b] - (deg * x1_ref[b] - off)

    stencil(w_ref, t2, col_ref, cnt_ref, hub_ref, rank_ref, hacc, second)
    pltpu.make_async_copy(ids_ref.at[pl.ds(0, 254)], ids_ref.at[pl.ds(0, 254)], idrs).wait()
    pltpu.make_async_copy(ids_ref.at[pl.ds(0, 254)], ids_ref.at[pl.ds(0, 254)], idss).wait()


def halo(columns, counts, lists, guess, rhs, degree, agg, weights):
    hbm = pl.BlockSpec(memory_space=pltpu.HBM)
    vm = pl.BlockSpec(memory_space=VMEM)
    sm = pl.BlockSpec(memory_space=SMEM)
    return pl.pallas_call(
        halo_kernel,
        out_shape=(
            jax.ShapeDtypeStruct((NB, BS, BS), f32),
            jax.ShapeDtypeStruct((NB, BS, BS), f32),
            jax.ShapeDtypeStruct((2 * ND, 1, BS), jnp.int32),
        ),
        in_specs=[sm, sm, sm, hbm, hbm, vm, vm, hbm],
        out_specs=(vm, vm, vm),
        scratch_shapes=[
            VMEM((NB, 16, BS, BS), bf16),
            VMEM((NB, BS, BS), f32),
            VMEM((NB, BS, BS), f32),
            VMEM((TB, BS, BS), bf16),
            VMEM((TB, BS, BS), bf16),
            VMEM((NB, BS, BS), bf16),
            VMEM((ND, 2, BS, BS), bf16),
            VMEM((ND, 2, 1, BS), jnp.int32),
            VMEM((HUBS, BS, BS), f32),
            SMEM((HUBS,), jnp.int32),
            SMEM((NB,), jnp.int32),
            pltpu.SemaphoreType.DMA((3,)),
            pltpu.SemaphoreType.DMA((2,)),
            pltpu.SemaphoreType.DMA((2,)),
            pltpu.SemaphoreType.DMA,
            pltpu.SemaphoreType.DMA,
        ],
        compiler_params=pltpu.CompilerParams(
            collective_id=0, has_side_effects=True, vmem_limit_bytes=60 * 2**20
        ),
        name="halo",
    )(columns, counts, lists, guess, rhs, degree, agg, weights)


def scatter_kernel(agg_ref, res_hbm, out_hbm, b0, b1, b2, b3, res_ref, rsem, osem):
    bufs = (b0, b1, b2, b3)
    n = 4096 // 4
    rcopy = pltpu.make_async_copy(res_hbm, res_ref, rsem)
    rcopy.start()

    def clear(i, _):
        for buf in bufs:
            for u in range(8):
                buf[pl.ds(i * 64 + u * 8, 8), :] = jnp.zeros((8, BS), f32)
        return 0

    lax.fori_loop(0, NC // 64, clear, 0)
    rcopy.wait()

    def add(i, _):
        for u in range(8):
            for q, buf in enumerate(bufs):
                r = q * n + i * 8 + u
                a = agg_ref[r]
                buf[pl.ds(a, 1), :] = buf[pl.ds(a, 1), :] + res_ref[pl.ds(r, 1), :]
        return 0

    lax.fori_loop(0, n // 8, add, 0)
    chunk = NC // 8
    outs = []
    for c in range(8):

        def total(i, _):
            for u in range(8):
                at = pl.ds(c * chunk + i * 64 + u * 8, 8)
                b0[at, :] = (b0[at, :] + b1[at, :]) + (b2[at, :] + b3[at, :])
            return 0

        lax.fori_loop(0, chunk // 64, total, 0)
        part = pl.ds(c * chunk, chunk)
        cp = pltpu.make_async_copy(b0.at[part, :], out_hbm.at[part, :], osem.at[c])
        outs.append(cp)
        if c:
            outs[c - 1].start()
    outs[-1].start()
    for cp in outs:
        cp.wait()


def scatter(agg, res):
    hbm = pl.BlockSpec(memory_space=pltpu.HBM)
    return pl.pallas_call(
        scatter_kernel,
        out_shape=jax.ShapeDtypeStruct((NC, BS), f32),
        in_specs=[pl.BlockSpec(memory_space=SMEM), hbm],
        out_specs=hbm,
        scratch_shapes=[VMEM((NC, BS), f32)] * 4
        + [VMEM((NB * BS, BS), f32), pltpu.SemaphoreType.DMA, pltpu.SemaphoreType.DMA((8,))],
        compiler_params=pltpu.CompilerParams(vmem_limit_bytes=63 * 2**20),
        name="scatter",
    )(agg, res)


UNIT = (32, 32, 16, 16, 16, 16)
PARTS = len(UNIT)
PACE = (2, 0, 1, 3, 4, 5)
BASE = tuple(64 * sum(UNIT[:p]) for p in range(PARTS))


def coarse_kernel(
    col_ref, cnt_ref, diag_ref, deg_ref, agg_hbm, ids_hbm, coarse_hbm, x1_hbm, res_hbm, w_hbm,
    out_ref,
    w_ref, x1_ref, res_ref, id0, id1, id2, id3, acc, swap, r1, r2, r3, corr, cf, table, pcl, tile0, tile1,
    hacc, hub_ref, rank_ref, lsem, isem, hsem, s0, q0, s1, q1, s2, q2, s3, q3,
    a3s, a3r, a2s, a2r, a1s, a1r, cs, cr,
):
    me, x, y, z, c = my_place()
    xyz = (x, y, z)
    half = c * HALF
    other = (1 - c) * HALF

    def along(dim, k):
        p = [x, y, z]
        p[dim] = lax.rem(p[dim] + k, 4)
        return place_id(p[0], p[1], p[2], c)

    partner = place_id(x, y, z, 1 - c)
    bar = pltpu.get_barrier_semaphore()
    pl.semaphore_signal(bar, inc=1, device_id=partner, device_id_type=MESH)
    for dim in range(3):
        for k in range(1, 4):
            pl.semaphore_signal(bar, inc=1, device_id=along(dim, k), device_id_type=MESH)

    def rcopy(src, dst, ssem, rsem, dev):
        return pltpu.make_async_remote_copy(src, dst, ssem, rsem, device_id=dev, device_id_type=MESH)

    def rows_at(at, rows):
        return pl.ds(pl.multiple_of(at, 16), rows)

    def add_into(dst, d0, srcs, rows, step=32):
        if rows % step:
            step = 16

        def go(i, _):
            v = dst[rows_at(d0 + i * step, step), :]
            for ref, r0 in srcs:
                v = v + ref[rows_at(r0 + i * step, step), :]
            dst[rows_at(d0 + i * step, step), :] = v
            return 0

        lax.fori_loop(0, rows // step, go, 0)

    order = ((0, 1, 2), (1, 2, 0), (2, 0, 1)) * (PARTS // 3)
    pieces = []
    for k, p in [(k, p + g) for g in range(0, PARTS, 3) for k in (1, 3, 2, 0) for p in range(3)]:
        rows = UNIT[p] * 16
        at = BASE[p] + lax.rem(xyz[order[p][0]] + k, 4) * rows
        hcopy = pltpu.make_async_copy(
            coarse_hbm.at[rows_at(half + at, rows), :], acc.at[rows_at(at, rows), :], hsem.at[p, k]
        )
        hcopy.start()
        pieces.append((k, p, at, rows, hcopy))
    pl.semaphore_wait(bar, 10)
    sends = []
    swaps = []
    for k, p, at, rows, hcopy in pieces:
        cp = rcopy(
            coarse_hbm.at[rows_at(other + at, rows), :], swap.at[rows_at(at, rows), :],
            s0.at[p, k], q0.at[p, k], partner,
        )
        cp.start()
        swaps.append(cp)
    loads = [
        pltpu.make_async_copy(src, dst, lsem.at[i])
        for i, (src, dst) in enumerate(
            ((w_hbm, w_ref), (x1_hbm, x1_ref), (res_hbm, res_ref))
        )
    ]
    pend = []
    sent1 = {}
    for (k, p, at, rows, hcopy), cp in zip(pieces, swaps):
        hcopy.wait()
        cp.wait_recv()
        add_into(acc, at, [(swap, at)], rows)
        if k:
            cp1 = rcopy(
                acc.at[rows_at(at, rows), :], r1.at[k - 1, pl.ds(BASE[p] // 4, rows), :],
                s1.at[p, k - 1], q1.at[p, k - 1], along(order[p][0], k),
            )
            sent1[p, k] = cp1
            pend.append(cp1)
        if len(pend) > 1:
            pend.pop(0).start()
    for cp1 in pend:
        cp1.start()
    for cp in loads:
        cp.start()
    find_hubs(cnt_ref, hub_ref, rank_ref)
    id_refs = (id0, id1, id2, id3)

    def fetch(src, n, g):
        part = src.at[pl.ds(pl.multiple_of(n * GROUP * BS, GROUP * BS), GROUP * BS)]
        return pltpu.make_async_copy(part, id_refs[g], isem.at[g])

    for g in range(2):
        fetch(agg_hbm, g, g).start()
        fetch(ids_hbm, g + 2, g + 2).start()
    cur = []
    sent2 = {}
    for p in PACE:
        rows = UNIT[p] * 16
        at = BASE[p] + xyz[order[p][0]] * rows
        for k in range(1, 4):
            sent1[p, k].wait_recv()
        add_into(acc, at, [(r1.at[k], BASE[p] // 4) for k in range(3)], rows)
        n2 = UNIT[p] * 4
        for k in range(1, 4):
            a = lax.rem(xyz[order[p][1]] + k, 4)
            sent2[p, k] = rcopy(
                acc.at[rows_at(at + a * n2, n2), :], r2.at[k - 1, pl.ds(BASE[p] // 16, n2), :],
                s2.at[p, k - 1], q2.at[p, k - 1], along(order[p][1], k),
            )
            sent2[p, k].start()
        cur.append((p, at + xyz[order[p][1]] * n2))
    sent3 = {}
    last = []
    for p, at in cur:
        rows = UNIT[p] * 4
        for k in range(1, 4):
            sent2[p, k].wait_recv()
        add_into(acc, at, [(r2.at[k], BASE[p] // 16) for k in range(3)], rows)
        n3 = UNIT[p]
        for k in range(1, 4):
            a = lax.rem(xyz[order[p][2]] + k, 4)
            sent3[p, k] = rcopy(
                acc.at[rows_at(at + a * n3, n3), :], r3.at[k - 1, pl.ds(BASE[p] // 64, n3), :],
                s3.at[p, k - 1], q3.at[p, k - 1], along(order[p][2], k),
            )
            sent3[p, k].start()
        last.append((p, at + xyz[order[p][2]] * n3))

    def spread(sent, p, dim, at, rows, ssem, rsem):
        for k in range(1, 4):
            ref = corr.at[rows_at(half + at, rows), :]
            cp = rcopy(ref, ref, ssem.at[p, k - 1], rsem.at[p, k - 1], along(dim, k))
            cp.start()
            sent[p, k] = cp
            sends.append(cp)

    def widen(at, rows):
        def go(i, _):
            here = rows_at(at + i * 16, 16)
            cf[here, :] = corr[here, :].astype(f32)
            return 0

        lax.fori_loop(0, rows // 16, go, 0)

    g3, g2, g1 = {}, {}, {}
    for p, at in last:
        rows = UNIT[p]
        for k in range(1, 4):
            sent3[p, k].wait_recv()
        for i in range(rows // 16):
            v = acc[rows_at(at + i * 16, 16), :]
            for k in range(3):
                v = v + r3[k, pl.ds(BASE[p] // 64 + i * 16, 16), :]
            div = jnp.concatenate(
                [jnp.full((1, BS), diag_ref[half + at + i * 16 + r], f32) for r in range(16)], axis=0
            )
            corr[rows_at(half + at + i * 16, 16), :] = (v / div).astype(bf16)
        spread(g3, p, order[p][2], at, rows, a3s, a3r)
    cur = []
    for p, at in last:
        for k in range(1, 4):
            g3[p, k].wait_recv()
        at = at - xyz[order[p][2]] * UNIT[p]
        cur.append((p, at))
        spread(g2, p, order[p][1], at, UNIT[p] * 4, a2s, a2r)
    swapped = []

    def hand_over(p, a, k):
        rows = UNIT[p] * 16
        ref = corr.at[rows_at(half + BASE[p] + a * rows, rows), :]
        cp = rcopy(ref, ref, cs.at[p, k], cr.at[p, k], partner)
        cp.start()
        sends.append(cp)
        swapped.append((cp, other + BASE[p] + a * rows, rows))
        widen(half + BASE[p] + a * rows, rows)

    for p, at in cur:
        for k in range(1, 4):
            g2[p, k].wait_recv()
        at = at - xyz[order[p][1]] * UNIT[p] * 4
        spread(g1, p, order[p][0], at, UNIT[p] * 16, a1s, a1r)
        hand_over(p, xyz[order[p][0]], 0)
    for k, p in [(k, p) for g in range(0, PARTS, 3) for k in (1, 3, 2) for p in PACE[g : g + 3]]:
        g1[p, k].wait_recv()
        hand_over(p, lax.rem(xyz[order[p][0]] + 4 - k, 4), k)
    for cp, at, rows in swapped:
        cp.wait_recv()
        widen(at, rows)
    for cp in loads:
        cp.wait()

    def local(i, _):
        for g in range(2):
            n = 2 * i + g
            fetch(agg_hbm, n, g).wait()
            for u in range(GROUP):
                b = n * GROUP + u
                for r in range(BS):
                    pcl[b, pl.ds(r, 1), :] = cf[pl.ds(id_refs[g][u * BS + r], 1), :]
                if u:
                    table[b - 1] = pcl[b - 1].astype(bf16)
            table[b] = pcl[b].astype(bf16)

            @pl.when(i == 0)
            def _():
                fetch(agg_hbm, n + 2, g).start()

        return 0

    lax.fori_loop(0, 2, local, 0)
    for g in range(2):
        fetch(ids_hbm, g, g).start()
    tiles = (tile0, tile1)

    def remote(i, _):
        for g in range(4):
            n = 4 * i + g
            fetch(ids_hbm, n, g).wait()
            for u in range(GROUP):
                t = NB + n * GROUP + u
                tile = tiles[u % 2]
                for r in range(BS):
                    tile[pl.ds(r, 1), :] = cf[pl.ds(id_refs[g][u * BS + r], 1), :]
                if u:
                    table[t - 1] = tiles[(u - 1) % 2][...].astype(bf16)
            table[t] = tile[...].astype(bf16)

            @pl.when(i < 2 * ND // GROUP // 4 - 1)
            def _():
                fetch(ids_hbm, n + 4, g).start()

        return 0

    lax.fori_loop(0, 2 * ND // GROUP // 4, remote, 0)

    def third(b, off):
        deg = column_of(deg_ref[b])
        pc = pcl[b]
        out_ref[b] = (x1_ref[b] + pc) + damping * (res_ref[b] - (deg * pc - off)) / deg

    stencil(w_ref, table, col_ref, cnt_ref, hub_ref, rank_ref, hacc, third)
    for cp in list(sent1.values()) + list(sent2.values()) + list(sent3.values()) + swaps + sends:
        cp.wait_send()


def coarse_leg(columns, counts, diag, degree, agg, ids, coarse, x1, res, weights):
    vm = pl.BlockSpec(memory_space=VMEM)
    sm = pl.BlockSpec(memory_space=SMEM)
    hbm = pl.BlockSpec(memory_space=pltpu.HBM)
    dma = pltpu.SemaphoreType.DMA
    return pl.pallas_call(
        coarse_kernel,
        out_shape=jax.ShapeDtypeStruct((NB, BS, BS), f32),
        in_specs=[sm, sm, sm, vm, hbm, hbm, hbm, hbm, hbm, hbm],
        out_specs=vm,
        scratch_shapes=[
            VMEM((NB, 16, BS, BS), bf16),
            VMEM((NB, BS, BS), f32),
            VMEM((NB, BS, BS), f32),
            SMEM((GROUP * BS,), jnp.int32),
            SMEM((GROUP * BS,), jnp.int32),
            SMEM((GROUP * BS,), jnp.int32),
            SMEM((GROUP * BS,), jnp.int32),
            VMEM((HALF, BS), f32),
            VMEM((HALF, BS), f32),
            VMEM((3, HALF // 4, BS), f32),
            VMEM((3, HALF // 16, BS), f32),
            VMEM((3, HALF // 64, BS), f32),
            VMEM((NC, BS), bf16),
            VMEM((NC, BS), f32),
            VMEM((TB, BS, BS), bf16),
            VMEM((NB, BS, BS), f32),
            VMEM((BS, BS), f32),
            VMEM((BS, BS), f32),
            VMEM((HUBS, BS, BS), f32),
            SMEM((HUBS,), jnp.int32),
            SMEM((NB,), jnp.int32),
            dma((3,)), dma((4,)),
            dma((PARTS, 4)), dma((PARTS, 4)), dma((PARTS, 4)),
            dma((PARTS, 3)), dma((PARTS, 3)), dma((PARTS, 3)), dma((PARTS, 3)), dma((PARTS, 3)), dma((PARTS, 3)),
            dma((PARTS, 3)), dma((PARTS, 3)), dma((PARTS, 3)), dma((PARTS, 3)), dma((PARTS, 3)), dma((PARTS, 3)),
            dma((PARTS, 4)), dma((PARTS, 4)),
        ],
        compiler_params=pltpu.CompilerParams(
            collective_id=1, has_side_effects=True, vmem_limit_bytes=63 * 2**20
        ),
        name="coarse_leg",
    )(columns, counts, diag, degree, agg, ids, coarse, x1, res, weights)


def body(rhs, guess, degree, weights, columns, block_counts, send_lists, aggregates, coarse_diag):
    cols = columns.T
    lists = send_lists[0].T
    deg = degree.reshape(NB, 1, BS)
    x1, res, ids = halo(
        cols, block_counts, lists,
        guess.reshape(NB, BS, BS), rhs.reshape(NB, BS, BS), deg,
        aggregates.reshape(NB, 1, BS), weights,
    )
    coarse = scatter(aggregates, res.reshape(NB * BS, BS))
    out = coarse_leg(
        cols, block_counts, coarse_diag, deg, aggregates, ids.reshape(-1), coarse, x1, res, weights
    )
    return out.reshape(NB * BS, BS)


def solution(mesh):
    both = ("rows", "cores")
    return jax.shard_map(
        body,
        mesh=mesh,
        in_specs=(
            P(both, None),
            P(both, None),
            P(both),
            P(both, None, None, None),
            P(both, None),
            P(both),
            P(both, None, None),
            P(both),
            P(),
        ),
        out_specs=P(both, None),
        check_vma=False,
    )
```

```python
import functools

import jax
import jax.numpy as jnp
from jax import lax
from jax.experimental import pallas as pl
from jax.experimental.pallas import tpu as pltpu
from jax.sharding import PartitionSpec as P

ND = 128
NB = 32
BS = 128
NC = 16384
HALF = NC // 2
TB = NB + 2 * ND
GROUP = 8
HUBS = 8
damping = 0.7
MESH = pl.DeviceIdType.MESH
VMEM = pltpu.VMEM
SMEM = pltpu.SMEM
f32 = jnp.float32
bf16 = jnp.bfloat16


def my_place():
    me = lax.axis_index("rows") * 4 + lax.axis_index("cores")
    return me, me // 32, lax.rem(me // 8, 4), lax.rem(me, 4), lax.rem(me // 4, 2)


def place_id(x, y, z, c):
    return ((x * 4 + y) * 2 + c, z)


def peer(k, spot):
    me, x, y, z, c = spot
    m = lax.rem(k * 19, 128)
    px = lax.rem(x + m // 32, 4)
    py = lax.rem(y + lax.rem(m // 8, 4), 4)
    pc = lax.rem(c + lax.rem(m // 4, 2), 2)
    pz = lax.rem(z + lax.rem(m, 4), 4)
    return px, py, pz, pc


def column_of(row):
    return jnp.broadcast_to(row, (BS, BS)).T


def find_hubs(cnt_ref, hub_ref, rank_ref):
    seen = jnp.int32(0)
    at = [jnp.int32(0)] * HUBS
    for b in range(NB):
        rank_ref[b] = seen
        seen = seen + jnp.where(cnt_ref[b] > 8, 1, 0)
        for k in range(HUBS):
            at[k] = at[k] + jnp.where(seen <= k, 1, 0)
    for k in range(HUBS):
        hub_ref[k] = jnp.minimum(at[k], NB - 1)


def half_row(w_ref, t_ref, col_ref, b, s0):
    acc = None
    for s in range(s0, s0 + 8, 2):
        lhs = jnp.concatenate([w_ref[b, s], w_ref[b, s + 1]], axis=1)
        rhs = jnp.concatenate([t_ref[col_ref[s, b]], t_ref[col_ref[s + 1, b]]], axis=0)
        part = jnp.dot(lhs, rhs, preferred_element_type=f32)
        acc = part if acc is None else acc + part
    return acc


def stencil(w_ref, t_ref, col_ref, cnt_ref, hub_ref, rank_ref, hacc, finish, width=4):
    def hubs(i, _):
        for u in range(width):
            k = i * width + u
            hacc[k] = half_row(w_ref, t_ref, col_ref, hub_ref[k], 8)
        return 0

    lax.fori_loop(0, HUBS // width, hubs, 0)

    def rows(i, _):
        for u in range(width):
            b = i * width + u
            extra = hacc[jnp.minimum(rank_ref[b], HUBS - 1)]
            off = half_row(w_ref, t_ref, col_ref, b, 0)
            off = off + jnp.where(cnt_ref[b] > 8, extra, 0.0)
            finish(b, off)
        return 0

    lax.fori_loop(0, NB // width, rows, 0)


def halo_kernel(
    col_ref, cnt_ref, lst_ref, guess_ref, rhs_ref, deg_ref, agg_ref, w_hbm,
    x1_ref, res_ref, ids_ref,
    w_ref, t1, t2, loc, sbuf, idbuf, hacc, hub_ref, rank_ref, wsem, ss, rs, idss, idrs,
):
    spot = my_place()
    me = spot[0]
    wcopy = pltpu.make_async_copy(w_hbm, w_ref, wsem)
    wcopy.start()
    bar = pltpu.get_barrier_semaphore()

    def hello(k, _):
        d = lax.rem(me + k, ND)
        pl.semaphore_signal(bar, inc=1, device_id=(d // 4, lax.rem(d, 4)), device_id_type=MESH)
        return 0

    lax.fori_loop(1, ND, hello, 0)

    def cast(b, _):
        v = guess_ref[b].astype(bf16)
        t1[b] = v
        loc[b] = v
        return 0

    lax.fori_loop(0, NB, cast, 0)

    def prepare(k, _):
        px, py, pz, pc = peer(k, spot)
        row = (px * 4 + py) * 2 + pc
        d = row * 4 + pz
        for j in range(2):
            own = lst_ref[j, d]
            sbuf[k, j] = loc[own]
            idbuf[k, j] = agg_ref[own]
        return 0

    lax.fori_loop(1, ND, prepare, 0)
    for j in range(2):
        own = lst_ref[j, me]
        t1[NB + 2 * me + j] = loc[own]
        ids_ref[2 * me + j] = agg_ref[own]
    pl.semaphore_wait(bar, ND - 1)

    def send(k, dst, i, dev):
        pltpu.make_async_remote_copy(
            sbuf.at[k], dst.at[pl.ds(NB + 2 * me, 2)], ss.at[i], rs.at[i],
            device_id=dev, device_id_type=MESH,
        ).start()

    def send1(k, _):
        px, py, pz, pc = peer(k, spot)
        dev = place_id(px, py, pz, pc)
        pltpu.make_async_remote_copy(
            idbuf.at[k], ids_ref.at[pl.ds(2 * me, 2)], idss, idrs,
            device_id=dev, device_id_type=MESH,
        ).start()
        send(k, t1, 0, dev)
        return 0

    lax.fori_loop(1, ND, send1, 0)
    find_hubs(cnt_ref, hub_ref, rank_ref)
    wcopy.wait()

    def wait_all(i):
        pltpu.make_async_copy(t1.at[pl.ds(0, 254)], t1.at[pl.ds(0, 254)], rs.at[i]).wait()
        pltpu.make_async_copy(t1.at[pl.ds(0, 254)], t1.at[pl.ds(0, 254)], ss.at[i]).wait()

    wait_all(0)

    def first(b, off):
        deg = column_of(deg_ref[b])
        g = guess_ref[b]
        x = g + damping * (rhs_ref[b] - (deg * g - off)) / deg
        x1_ref[b] = x
        v = x.astype(bf16)
        t2[b] = v
        loc[b] = v

    stencil(w_ref, t1, col_ref, cnt_ref, hub_ref, rank_ref, hacc, first)

    def fill2(k, _):
        px, py, pz, pc = peer(k, spot)
        d = ((px * 4 + py) * 2 + pc) * 4 + pz
        for j in range(2):
            sbuf[k, j] = loc[lst_ref[j, d]]

        @pl.when(k > 2)
        def _():
            send(k - 2, t2, 1, place_id(*peer(k - 2, spot)))

        return 0

    lax.fori_loop(1, ND, fill2, 0)
    send(ND - 2, t2, 1, place_id(*peer(ND - 2, spot)))
    for j in range(2):
        t2[NB + 2 * me + j] = loc[lst_ref[j, me]]
    send(ND - 1, t2, 1, place_id(*peer(ND - 1, spot)))
    wait_all(1)

    def second(b, off):
        deg = column_of(deg_ref[b])
        res_ref[b] = rhs_ref[b] - (deg * x1_ref[b] - off)

    stencil(w_ref, t2, col_ref, cnt_ref, hub_ref, rank_ref, hacc, second)
    pltpu.make_async_copy(ids_ref.at[pl.ds(0, 254)], ids_ref.at[pl.ds(0, 254)], idrs).wait()
    pltpu.make_async_copy(ids_ref.at[pl.ds(0, 254)], ids_ref.at[pl.ds(0, 254)], idss).wait()


def halo(columns, counts, lists, guess, rhs, degree, agg, weights):
    vm = pl.BlockSpec(memory_space=VMEM)
    sm = pl.BlockSpec(memory_space=SMEM)
    return pl.pallas_call(
        halo_kernel,
        out_shape=(
            jax.ShapeDtypeStruct((NB, BS, BS), f32),
            jax.ShapeDtypeStruct((NB, BS, BS), f32),
            jax.ShapeDtypeStruct((2 * ND, 1, BS), jnp.int32),
        ),
        in_specs=[sm, sm, sm, vm, vm, vm, vm, pl.BlockSpec(memory_space=pl.ANY)],
        out_specs=(vm, vm, vm),
        scratch_shapes=[
            VMEM((NB, 16, BS, BS), bf16),
            VMEM((TB, BS, BS), bf16),
            VMEM((TB, BS, BS), bf16),
            VMEM((NB, BS, BS), bf16),
            VMEM((ND, 2, BS, BS), bf16),
            VMEM((ND, 2, 1, BS), jnp.int32),
            VMEM((HUBS, BS, BS), f32),
            SMEM((HUBS,), jnp.int32),
            SMEM((NB,), jnp.int32),
            pltpu.SemaphoreType.DMA,
            pltpu.SemaphoreType.DMA((2,)),
            pltpu.SemaphoreType.DMA((2,)),
            pltpu.SemaphoreType.DMA,
            pltpu.SemaphoreType.DMA,
        ],
        compiler_params=pltpu.CompilerParams(
            collective_id=0, has_side_effects=True, vmem_limit_bytes=60 * 2**20
        ),
        name="halo",
    )(columns, counts, lists, guess, rhs, degree, agg, weights)


def scatter_kernel(agg_ref, res_hbm, out_hbm, b0, b1, b2, b3, res_ref, rsem, osem):
    bufs = (b0, b1, b2, b3)
    n = 4096 // 4
    rcopy = pltpu.make_async_copy(res_hbm, res_ref, rsem)
    rcopy.start()

    def clear(i, _):
        for buf in bufs:
            for u in range(8):
                buf[pl.ds(i * 64 + u * 8, 8), :] = jnp.zeros((8, BS), f32)
        return 0

    lax.fori_loop(0, NC // 64, clear, 0)
    rcopy.wait()

    def add(i, _):
        for u in range(8):
            for q, buf in enumerate(bufs):
                r = q * n + i * 8 + u
                a = agg_ref[r]
                buf[pl.ds(a, 1), :] = buf[pl.ds(a, 1), :] + res_ref[pl.ds(r, 1), :]
        return 0

    lax.fori_loop(0, n // 8, add, 0)
    chunk = NC // 8
    outs = []
    for c in range(8):

        def total(i, _):
            for u in range(8):
                at = pl.ds(c * chunk + i * 64 + u * 8, 8)
                b0[at, :] = (b0[at, :] + b1[at, :]) + (b2[at, :] + b3[at, :])
            return 0

        lax.fori_loop(0, chunk // 64, total, 0)
        part = pl.ds(c * chunk, chunk)
        cp = pltpu.make_async_copy(b0.at[part, :], out_hbm.at[part, :], osem.at[c])
        outs.append(cp)
        if c:
            outs[c - 1].start()
    outs[-1].start()
    for cp in outs:
        cp.wait()


def scatter(agg, res):
    hbm = pl.BlockSpec(memory_space=pltpu.HBM)
    return pl.pallas_call(
        scatter_kernel,
        out_shape=jax.ShapeDtypeStruct((NC, BS), f32),
        in_specs=[pl.BlockSpec(memory_space=SMEM), hbm],
        out_specs=hbm,
        scratch_shapes=[VMEM((NC, BS), f32)] * 4
        + [VMEM((NB * BS, BS), f32), pltpu.SemaphoreType.DMA, pltpu.SemaphoreType.DMA((8,))],
        compiler_params=pltpu.CompilerParams(vmem_limit_bytes=63 * 2**20),
        name="scatter",
    )(agg, res)


UNIT = (32, 32, 16, 16, 16, 16)
PARTS = len(UNIT)
PACE = (2, 0, 1, 3, 4, 5)
BASE = tuple(64 * sum(UNIT[:p]) for p in range(PARTS))


def coarse_kernel(
    col_ref, cnt_ref, diag_ref, deg_ref, agg_hbm, ids_hbm, coarse_hbm, x1_hbm, res_hbm, w_hbm,
    out_ref,
    w_ref, x1_ref, res_ref, id0, id1, id2, id3, acc, swap, r1, r2, r3, corr, cf, table, pcl, tile0, tile1,
    hacc, hub_ref, rank_ref, lsem, isem, hsem, s0, q0, s1, q1, s2, q2, s3, q3,
    a3s, a3r, a2s, a2r, a1s, a1r, cs, cr,
):
    me, x, y, z, c = my_place()
    xyz = (x, y, z)
    half = c * HALF
    other = (1 - c) * HALF

    def along(dim, k):
        p = [x, y, z]
        p[dim] = lax.rem(p[dim] + k, 4)
        return place_id(p[0], p[1], p[2], c)

    partner = place_id(x, y, z, 1 - c)
    bar = pltpu.get_barrier_semaphore()
    pl.semaphore_signal(bar, inc=1, device_id=partner, device_id_type=MESH)
    for dim in range(3):
        for k in range(1, 4):
            pl.semaphore_signal(bar, inc=1, device_id=along(dim, k), device_id_type=MESH)

    def rcopy(src, dst, ssem, rsem, dev):
        return pltpu.make_async_remote_copy(src, dst, ssem, rsem, device_id=dev, device_id_type=MESH)

    def rows_at(at, rows):
        return pl.ds(pl.multiple_of(at, 16), rows)

    def add_into(dst, d0, srcs, rows, step=32):
        if rows % step:
            step = 16

        def go(i, _):
            v = dst[rows_at(d0 + i * step, step), :]
            for ref, r0 in srcs:
                v = v + ref[rows_at(r0 + i * step, step), :]
            dst[rows_at(d0 + i * step, step), :] = v
            return 0

        lax.fori_loop(0, rows // step, go, 0)

    order = ((0, 1, 2), (1, 2, 0), (2, 0, 1)) * (PARTS // 3)
    pieces = []
    for k, p in [(k, p + g) for g in range(0, PARTS, 3) for k in (1, 3, 2, 0) for p in range(3)]:
        rows = UNIT[p] * 16
        at = BASE[p] + lax.rem(xyz[order[p][0]] + k, 4) * rows
        hcopy = pltpu.make_async_copy(
            coarse_hbm.at[rows_at(half + at, rows), :], acc.at[rows_at(at, rows), :], hsem.at[p, k]
        )
        hcopy.start()
        pieces.append((k, p, at, rows, hcopy))
    pl.semaphore_wait(bar, 10)
    sends = []
    swaps = []
    for k, p, at, rows, hcopy in pieces:
        cp = rcopy(
            coarse_hbm.at[rows_at(other + at, rows), :], swap.at[rows_at(at, rows), :],
            s0.at[p, k], q0.at[p, k], partner,
        )
        cp.start()
        swaps.append(cp)
    loads = [
        pltpu.make_async_copy(src, dst, lsem.at[i])
        for i, (src, dst) in enumerate(
            ((w_hbm, w_ref), (x1_hbm, x1_ref), (res_hbm, res_ref))
        )
    ]
    pend = []
    sent1 = {}
    for (k, p, at, rows, hcopy), cp in zip(pieces, swaps):
        hcopy.wait()
        cp.wait_recv()
        add_into(acc, at, [(swap, at)], rows)
        if k:
            cp1 = rcopy(
                acc.at[rows_at(at, rows), :], r1.at[k - 1, pl.ds(BASE[p] // 4, rows), :],
                s1.at[p, k - 1], q1.at[p, k - 1], along(order[p][0], k),
            )
            sent1[p, k] = cp1
            pend.append(cp1)
        if len(pend) > 1:
            pend.pop(0).start()
    for cp1 in pend:
        cp1.start()
    for cp in loads:
        cp.start()
    find_hubs(cnt_ref, hub_ref, rank_ref)
    id_refs = (id0, id1, id2, id3)

    def fetch(src, n, g):
        part = src.at[pl.ds(pl.multiple_of(n * GROUP * BS, GROUP * BS), GROUP * BS)]
        return pltpu.make_async_copy(part, id_refs[g], isem.at[g])

    for g in range(2):
        fetch(agg_hbm, g, g).start()
        fetch(ids_hbm, g + 2, g + 2).start()
    cur = []
    sent2 = {}
    for p in PACE:
        rows = UNIT[p] * 16
        at = BASE[p] + xyz[order[p][0]] * rows
        for k in range(1, 4):
            sent1[p, k].wait_recv()
        add_into(acc, at, [(r1.at[k], BASE[p] // 4) for k in range(3)], rows)
        n2 = UNIT[p] * 4
        for k in range(1, 4):
            a = lax.rem(xyz[order[p][1]] + k, 4)
            sent2[p, k] = rcopy(
                acc.at[rows_at(at + a * n2, n2), :], r2.at[k - 1, pl.ds(BASE[p] // 16, n2), :],
                s2.at[p, k - 1], q2.at[p, k - 1], along(order[p][1], k),
            )
            sent2[p, k].start()
        cur.append((p, at + xyz[order[p][1]] * n2))
    sent3 = {}
    last = []
    for p, at in cur:
        rows = UNIT[p] * 4
        for k in range(1, 4):
            sent2[p, k].wait_recv()
        add_into(acc, at, [(r2.at[k], BASE[p] // 16) for k in range(3)], rows)
        n3 = UNIT[p]
        for k in range(1, 4):
            a = lax.rem(xyz[order[p][2]] + k, 4)
            sent3[p, k] = rcopy(
                acc.at[rows_at(at + a * n3, n3), :], r3.at[k - 1, pl.ds(BASE[p] // 64, n3), :],
                s3.at[p, k - 1], q3.at[p, k - 1], along(order[p][2], k),
            )
            sent3[p, k].start()
        last.append((p, at + xyz[order[p][2]] * n3))

    def spread(sent, p, dim, at, rows, ssem, rsem):
        for k in range(1, 4):
            ref = corr.at[rows_at(half + at, rows), :]
            cp = rcopy(ref, ref, ssem.at[p, k - 1], rsem.at[p, k - 1], along(dim, k))
            cp.start()
            sent[p, k] = cp
            sends.append(cp)

    def widen(at, rows):
        def go(i, _):
            here = rows_at(at + i * 16, 16)
            cf[here, :] = corr[here, :].astype(f32)
            return 0

        lax.fori_loop(0, rows // 16, go, 0)

    g3, g2, g1 = {}, {}, {}
    for p, at in last:
        rows = UNIT[p]
        for k in range(1, 4):
            sent3[p, k].wait_recv()
        for i in range(rows // 16):
            v = acc[rows_at(at + i * 16, 16), :]
            for k in range(3):
                v = v + r3[k, pl.ds(BASE[p] // 64 + i * 16, 16), :]
            div = jnp.concatenate(
                [jnp.full((1, BS), diag_ref[half + at + i * 16 + r], f32) for r in range(16)], axis=0
            )
            corr[rows_at(half + at + i * 16, 16), :] = (v / div).astype(bf16)
        spread(g3, p, order[p][2], at, rows, a3s, a3r)
    cur = []
    for p, at in last:
        for k in range(1, 4):
            g3[p, k].wait_recv()
        at = at - xyz[order[p][2]] * UNIT[p]
        cur.append((p, at))
        spread(g2, p, order[p][1], at, UNIT[p] * 4, a2s, a2r)
    swapped = []

    def hand_over(p, a, k):
        rows = UNIT[p] * 16
        ref = corr.at[rows_at(half + BASE[p] + a * rows, rows), :]
        cp = rcopy(ref, ref, cs.at[p, k], cr.at[p, k], partner)
        cp.start()
        sends.append(cp)
        swapped.append((cp, other + BASE[p] + a * rows, rows))
        widen(half + BASE[p] + a * rows, rows)

    for p, at in cur:
        for k in range(1, 4):
            g2[p, k].wait_recv()
        at = at - xyz[order[p][1]] * UNIT[p] * 4
        spread(g1, p, order[p][0], at, UNIT[p] * 16, a1s, a1r)
        hand_over(p, xyz[order[p][0]], 0)
    for k, p in [(k, p) for g in range(0, PARTS, 3) for k in (1, 3, 2) for p in PACE[g : g + 3]]:
        g1[p, k].wait_recv()
        hand_over(p, lax.rem(xyz[order[p][0]] + 4 - k, 4), k)
    for cp, at, rows in swapped:
        cp.wait_recv()
        widen(at, rows)
    for cp in loads:
        cp.wait()

    def local(i, _):
        for g in range(2):
            n = 2 * i + g
            fetch(agg_hbm, n, g).wait()
            for u in range(GROUP):
                b = n * GROUP + u
                for r in range(BS):
                    pcl[b, pl.ds(r, 1), :] = cf[pl.ds(id_refs[g][u * BS + r], 1), :]
                if u:
                    table[b - 1] = pcl[b - 1].astype(bf16)
            table[b] = pcl[b].astype(bf16)

            @pl.when(i == 0)
            def _():
                fetch(agg_hbm, n + 2, g).start()

        return 0

    lax.fori_loop(0, 2, local, 0)
    for g in range(2):
        fetch(ids_hbm, g, g).start()
    tiles = (tile0, tile1)

    def remote(i, _):
        for g in range(4):
            n = 4 * i + g
            fetch(ids_hbm, n, g).wait()
            for u in range(GROUP):
                t = NB + n * GROUP + u
                tile = tiles[u % 2]
                for r in range(BS):
                    tile[pl.ds(r, 1), :] = cf[pl.ds(id_refs[g][u * BS + r], 1), :]
                if u:
                    table[t - 1] = tiles[(u - 1) % 2][...].astype(bf16)
            table[t] = tile[...].astype(bf16)

            @pl.when(i < 2 * ND // GROUP // 4 - 1)
            def _():
                fetch(ids_hbm, n + 4, g).start()

        return 0

    lax.fori_loop(0, 2 * ND // GROUP // 4, remote, 0)

    def third(b, off):
        deg = column_of(deg_ref[b])
        pc = pcl[b]
        out_ref[b] = (x1_ref[b] + pc) + damping * (res_ref[b] - (deg * pc - off)) / deg

    stencil(w_ref, table, col_ref, cnt_ref, hub_ref, rank_ref, hacc, third)
    for cp in list(sent1.values()) + list(sent2.values()) + list(sent3.values()) + swaps + sends:
        cp.wait_send()


def coarse_leg(columns, counts, diag, degree, agg, ids, coarse, x1, res, weights):
    vm = pl.BlockSpec(memory_space=VMEM)
    sm = pl.BlockSpec(memory_space=SMEM)
    hbm = pl.BlockSpec(memory_space=pltpu.HBM)
    dma = pltpu.SemaphoreType.DMA
    return pl.pallas_call(
        coarse_kernel,
        out_shape=VMEM((NB, BS, BS), f32),
        in_specs=[sm, sm, sm, vm, hbm, hbm, hbm, hbm, hbm, hbm],
        out_specs=vm,
        scratch_shapes=[
            VMEM((NB, 16, BS, BS), bf16),
            VMEM((NB, BS, BS), f32),
            VMEM((NB, BS, BS), f32),
            SMEM((GROUP * BS,), jnp.int32),
            SMEM((GROUP * BS,), jnp.int32),
            SMEM((GROUP * BS,), jnp.int32),
            SMEM((GROUP * BS,), jnp.int32),
            VMEM((HALF, BS), f32),
            VMEM((HALF, BS), f32),
            VMEM((3, HALF // 4, BS), f32),
            VMEM((3, HALF // 16, BS), f32),
            VMEM((3, HALF // 64, BS), f32),
            VMEM((NC, BS), bf16),
            VMEM((NC, BS), f32),
            VMEM((TB, BS, BS), bf16),
            VMEM((NB, BS, BS), f32),
            VMEM((BS, BS), f32),
            VMEM((BS, BS), f32),
            VMEM((HUBS, BS, BS), f32),
            SMEM((HUBS,), jnp.int32),
            SMEM((NB,), jnp.int32),
            dma((3,)), dma((4,)),
            dma((PARTS, 4)), dma((PARTS, 4)), dma((PARTS, 4)),
            dma((PARTS, 3)), dma((PARTS, 3)), dma((PARTS, 3)), dma((PARTS, 3)), dma((PARTS, 3)), dma((PARTS, 3)),
            dma((PARTS, 3)), dma((PARTS, 3)), dma((PARTS, 3)), dma((PARTS, 3)), dma((PARTS, 3)), dma((PARTS, 3)),
            dma((PARTS, 4)), dma((PARTS, 4)),
        ],
        compiler_params=pltpu.CompilerParams(
            collective_id=1, has_side_effects=True, vmem_limit_bytes=60 * 2**20
        ),
        name="coarse_leg",
    )(columns, counts, diag, degree, agg, ids, coarse, x1, res, weights)


def body(rhs, guess, degree, weights, columns, block_counts, send_lists, aggregates, coarse_diag):
    cols = columns.T
    lists = send_lists[0].T
    deg = degree.reshape(NB, 1, BS)
    x1, res, ids = halo(
        cols, block_counts, lists,
        guess.reshape(NB, BS, BS), rhs.reshape(NB, BS, BS), deg,
        aggregates.reshape(NB, 1, BS), weights,
    )
    coarse = scatter(aggregates, res.reshape(NB * BS, BS))
    out = coarse_leg(
        cols, block_counts, coarse_diag, deg, aggregates, ids.reshape(-1), coarse, x1, res, weights
    )
    return out.reshape(NB * BS, BS)


def solution(mesh):
    both = ("rows", "cores")
    return jax.shard_map(
        body,
        mesh=mesh,
        in_specs=(
            P(both, None),
            P(both, None),
            P(both),
            P(both, None, None, None),
            P(both, None),
            P(both),
            P(both, None, None),
            P(both),
            P(),
        ),
        out_specs=P(both, None),
        check_vma=False,
    )
```

```python
import functools

import jax
import jax.numpy as jnp
from jax import lax
from jax.experimental import pallas as pl
from jax.experimental.pallas import tpu as pltpu
from jax.sharding import PartitionSpec as P

ND = 128
NB = 32
BS = 128
NC = 16384
HALF = NC // 2
TB = NB + 2 * ND
GROUP = 8
HUBS = 8
damping = 0.7
MESH = pl.DeviceIdType.MESH
VMEM = pltpu.VMEM
SMEM = pltpu.SMEM
f32 = jnp.float32
bf16 = jnp.bfloat16


def my_place():
    me = lax.axis_index("rows") * 4 + lax.axis_index("cores")
    return me, me // 32, lax.rem(me // 8, 4), lax.rem(me, 4), lax.rem(me // 4, 2)


def place_id(x, y, z, c):
    return ((x * 4 + y) * 2 + c, z)


def peer(k, spot):
    me, x, y, z, c = spot
    m = lax.rem(k * 19, 128)
    px = lax.rem(x + m // 32, 4)
    py = lax.rem(y + lax.rem(m // 8, 4), 4)
    pc = lax.rem(c + lax.rem(m // 4, 2), 2)
    pz = lax.rem(z + lax.rem(m, 4), 4)
    return px, py, pz, pc


def column_of(row):
    return jnp.broadcast_to(row, (BS, BS)).T


def find_hubs(cnt_ref, hub_ref, rank_ref):
    seen = jnp.int32(0)
    at = [jnp.int32(0)] * HUBS
    for b in range(NB):
        rank_ref[b] = seen
        seen = seen + jnp.where(cnt_ref[b] > 8, 1, 0)
        for k in range(HUBS):
            at[k] = at[k] + jnp.where(seen <= k, 1, 0)
    for k in range(HUBS):
        hub_ref[k] = jnp.minimum(at[k], NB - 1)


def half_row(w_ref, t_ref, col_ref, b, s0):
    acc = None
    for s in range(s0, s0 + 8, 2):
        lhs = jnp.concatenate([w_ref[b, s], w_ref[b, s + 1]], axis=1)
        rhs = jnp.concatenate([t_ref[col_ref[s, b]], t_ref[col_ref[s + 1, b]]], axis=0)
        part = jnp.dot(lhs, rhs, preferred_element_type=f32)
        acc = part if acc is None else acc + part
    return acc


def stencil(w_ref, t_ref, col_ref, cnt_ref, hub_ref, rank_ref, hacc, finish, width=8):
    def hubs(i, _):
        for u in range(width):
            k = i * width + u
            hacc[k] = half_row(w_ref, t_ref, col_ref, hub_ref[k], 8)
        return 0

    lax.fori_loop(0, HUBS // width, hubs, 0)

    def rows(i, _):
        for u in range(width):
            b = i * width + u
            extra = hacc[jnp.minimum(rank_ref[b], HUBS - 1)]
            off = half_row(w_ref, t_ref, col_ref, b, 0)
            off = off + jnp.where(cnt_ref[b] > 8, extra, 0.0)
            finish(b, off)
        return 0

    lax.fori_loop(0, NB // width, rows, 0)


def halo_kernel(
    col_ref, cnt_ref, lst_ref, guess_ref, rhs_ref, deg_ref, agg_ref, w_hbm,
    x1_hbm, res_ref, ids_ref,
    w_ref, x1_ref, t1, t2, loc, sbuf, idbuf, hacc, hub_ref, rank_ref, wsem, xsem, ss, rs, idss, idrs,
):
    spot = my_place()
    me = spot[0]
    wcopy = pltpu.make_async_copy(w_hbm, w_ref, wsem)
    wcopy.start()
    bar = pltpu.get_barrier_semaphore()

    def hello(k, _):
        d = lax.rem(me + k, ND)
        pl.semaphore_signal(bar, inc=1, device_id=(d // 4, lax.rem(d, 4)), device_id_type=MESH)
        return 0

    lax.fori_loop(1, ND, hello, 0)

    def cast(b, _):
        v = guess_ref[b].astype(bf16)
        t1[b] = v
        loc[b] = v
        return 0

    lax.fori_loop(0, NB, cast, 0)

    def prepare(k, _):
        px, py, pz, pc = peer(k, spot)
        row = (px * 4 + py) * 2 + pc
        d = row * 4 + pz
        for j in range(2):
            own = lst_ref[j, d]
            sbuf[k, j] = loc[own]
            idbuf[k, j] = agg_ref[own]
        return 0

    lax.fori_loop(1, ND, prepare, 0)
    for j in range(2):
        own = lst_ref[j, me]
        t1[NB + 2 * me + j] = loc[own]
        ids_ref[2 * me + j] = agg_ref[own]
    pl.semaphore_wait(bar, ND - 1)

    def send(k, dst, i, dev):
        pltpu.make_async_remote_copy(
            sbuf.at[k], dst.at[pl.ds(NB + 2 * me, 2)], ss.at[i], rs.at[i],
            device_id=dev, device_id_type=MESH,
        ).start()

    def send1(k, _):
        px, py, pz, pc = peer(k, spot)
        dev = place_id(px, py, pz, pc)
        pltpu.make_async_remote_copy(
            idbuf.at[k], ids_ref.at[pl.ds(2 * me, 2)], idss, idrs,
            device_id=dev, device_id_type=MESH,
        ).start()
        send(k, t1, 0, dev)
        return 0

    lax.fori_loop(1, ND, send1, 0)
    find_hubs(cnt_ref, hub_ref, rank_ref)
    wcopy.wait()

    def wait_all(i):
        pltpu.make_async_copy(t1.at[pl.ds(0, 254)], t1.at[pl.ds(0, 254)], rs.at[i]).wait()
        pltpu.make_async_copy(t1.at[pl.ds(0, 254)], t1.at[pl.ds(0, 254)], ss.at[i]).wait()

    wait_all(0)

    def first(b, off):
        deg = column_of(deg_ref[b])
        g = guess_ref[b]
        x = g + damping * (rhs_ref[b] - (deg * g - off)) / deg
        x1_ref[b] = x
        v = x.astype(bf16)
        t2[b] = v
        loc[b] = v

    stencil(w_ref, t1, col_ref, cnt_ref, hub_ref, rank_ref, hacc, first)

    def fill2(k, _):
        px, py, pz, pc = peer(k, spot)
        d = ((px * 4 + py) * 2 + pc) * 4 + pz
        for j in range(2):
            sbuf[k, j] = loc[lst_ref[j, d]]

        @pl.when(k > 2)
        def _():
            send(k - 2, t2, 1, place_id(*peer(k - 2, spot)))

        return 0

    lax.fori_loop(1, ND, fill2, 0)
    send(ND - 2, t2, 1, place_id(*peer(ND - 2, spot)))
    for j in range(2):
        t2[NB + 2 * me + j] = loc[lst_ref[j, me]]
    send(ND - 1, t2, 1, place_id(*peer(ND - 1, spot)))
    x1_copy = pltpu.make_async_copy(x1_ref, x1_hbm, xsem)
    x1_copy.start()
    wait_all(1)

    def second(b, off):
        deg = column_of(deg_ref[b])
        res_ref[b] = rhs_ref[b] - (deg * x1_ref[b] - off)

    stencil(w_ref, t2, col_ref, cnt_ref, hub_ref, rank_ref, hacc, second)
    x1_copy.wait()
    pltpu.make_async_copy(ids_ref.at[pl.ds(0, 254)], ids_ref.at[pl.ds(0, 254)], idrs).wait()
    pltpu.make_async_copy(ids_ref.at[pl.ds(0, 254)], ids_ref.at[pl.ds(0, 254)], idss).wait()


def halo(columns, counts, lists, guess, rhs, degree, agg, weights):
    vm = pl.BlockSpec(memory_space=VMEM)
    sm = pl.BlockSpec(memory_space=SMEM)
    return pl.pallas_call(
        halo_kernel,
        out_shape=(
            jax.ShapeDtypeStruct((NB, BS, BS), f32),
            jax.ShapeDtypeStruct((NB, BS, BS), f32),
            jax.ShapeDtypeStruct((2 * ND, 1, BS), jnp.int32),
        ),
        in_specs=[sm, sm, sm, vm, vm, vm, vm, pl.BlockSpec(memory_space=pl.ANY)],
        out_specs=(pl.BlockSpec(memory_space=pltpu.HBM), vm, vm),
        scratch_shapes=[
            VMEM((NB, 16, BS, BS), bf16),
            VMEM((NB, BS, BS), f32),
            VMEM((TB, BS, BS), bf16),
            VMEM((TB, BS, BS), bf16),
            VMEM((NB, BS, BS), bf16),
            VMEM((ND, 2, BS, BS), bf16),
            VMEM((ND, 2, 1, BS), jnp.int32),
            VMEM((HUBS, BS, BS), f32),
            SMEM((HUBS,), jnp.int32),
            SMEM((NB,), jnp.int32),
            pltpu.SemaphoreType.DMA,
            pltpu.SemaphoreType.DMA,
            pltpu.SemaphoreType.DMA((2,)),
            pltpu.SemaphoreType.DMA((2,)),
            pltpu.SemaphoreType.DMA,
            pltpu.SemaphoreType.DMA,
        ],
        compiler_params=pltpu.CompilerParams(
            collective_id=0, has_side_effects=True, vmem_limit_bytes=60 * 2**20
        ),
        name="halo",
    )(columns, counts, lists, guess, rhs, degree, agg, weights)


def scatter_kernel(agg_ref, res_hbm, out_hbm, b0, b1, b2, b3, res_ref, rsem, osem):
    bufs = (b0, b1, b2, b3)
    n = 4096 // 4
    rcopy = pltpu.make_async_copy(res_hbm, res_ref, rsem)
    rcopy.start()

    def clear(i, _):
        for buf in bufs:
            for u in range(8):
                buf[pl.ds(i * 64 + u * 8, 8), :] = jnp.zeros((8, BS), f32)
        return 0

    lax.fori_loop(0, NC // 64, clear, 0)
    rcopy.wait()

    def add(i, _):
        for u in range(8):
            for q, buf in enumerate(bufs):
                r = q * n + i * 8 + u
                a = agg_ref[r]
                buf[pl.ds(a, 1), :] = buf[pl.ds(a, 1), :] + res_ref[pl.ds(r, 1), :]
        return 0

    lax.fori_loop(0, n // 8, add, 0)
    chunk = NC // 8
    outs = []
    for c in range(8):

        def total(i, _):
            for u in range(8):
                at = pl.ds(c * chunk + i * 64 + u * 8, 8)
                b0[at, :] = (b0[at, :] + b1[at, :]) + (b2[at, :] + b3[at, :])
            return 0

        lax.fori_loop(0, chunk // 64, total, 0)
        part = pl.ds(c * chunk, chunk)
        cp = pltpu.make_async_copy(b0.at[part, :], out_hbm.at[part, :], osem.at[c])
        outs.append(cp)
        if c:
            outs[c - 1].start()
    outs[-1].start()
    for cp in outs:
        cp.wait()


def scatter(agg, res):
    hbm = pl.BlockSpec(memory_space=pltpu.HBM)
    return pl.pallas_call(
        scatter_kernel,
        out_shape=jax.ShapeDtypeStruct((NC, BS), f32),
        in_specs=[pl.BlockSpec(memory_space=SMEM), hbm],
        out_specs=hbm,
        scratch_shapes=[VMEM((NC, BS), f32)] * 4
        + [VMEM((NB * BS, BS), f32), pltpu.SemaphoreType.DMA, pltpu.SemaphoreType.DMA((8,))],
        compiler_params=pltpu.CompilerParams(vmem_limit_bytes=63 * 2**20),
        name="scatter",
    )(agg, res)


UNIT = (32, 32, 16, 16, 16, 16)
PARTS = len(UNIT)
PACE = (2, 0, 1, 3, 4, 5)
BASE = tuple(64 * sum(UNIT[:p]) for p in range(PARTS))


def coarse_kernel(
    col_ref, cnt_ref, diag_ref, deg_ref, agg_hbm, ids_hbm, coarse_hbm, x1_hbm, res_hbm, w_hbm,
    out_ref,
    w_ref, x1_ref, res_ref, id0, id1, id2, id3, acc, swap, r1, r2, r3, corr, cf, table, pcl, tile0, tile1,
    hacc, hub_ref, rank_ref, lsem, isem, hsem, s0, q0, s1, q1, s2, q2, s3, q3,
    a3s, a3r, a2s, a2r, a1s, a1r, cs, cr,
):
    me, x, y, z, c = my_place()
    xyz = (x, y, z)
    half = c * HALF
    other = (1 - c) * HALF

    def along(dim, k):
        p = [x, y, z]
        p[dim] = lax.rem(p[dim] + k, 4)
        return place_id(p[0], p[1], p[2], c)

    partner = place_id(x, y, z, 1 - c)
    bar = pltpu.get_barrier_semaphore()
    pl.semaphore_signal(bar, inc=1, device_id=partner, device_id_type=MESH)
    for dim in range(3):
        for k in range(1, 4):
            pl.semaphore_signal(bar, inc=1, device_id=along(dim, k), device_id_type=MESH)

    def rcopy(src, dst, ssem, rsem, dev):
        return pltpu.make_async_remote_copy(src, dst, ssem, rsem, device_id=dev, device_id_type=MESH)

    def rows_at(at, rows):
        return pl.ds(pl.multiple_of(at, 16), rows)

    def add_into(dst, d0, srcs, rows, step=32):
        if rows % step:
            step = 16

        def go(i, _):
            v = dst[rows_at(d0 + i * step, step), :]
            for ref, r0 in srcs:
                v = v + ref[rows_at(r0 + i * step, step), :]
            dst[rows_at(d0 + i * step, step), :] = v
            return 0

        lax.fori_loop(0, rows // step, go, 0)

    order = ((0, 1, 2), (1, 2, 0), (2, 0, 1)) * (PARTS // 3)
    pieces = []
    for k, p in [(k, p + g) for g in range(0, PARTS, 3) for k in (1, 3, 2, 0) for p in range(3)]:
        rows = UNIT[p] * 16
        at = BASE[p] + lax.rem(xyz[order[p][0]] + k, 4) * rows
        hcopy = pltpu.make_async_copy(
            coarse_hbm.at[rows_at(half + at, rows), :], acc.at[rows_at(at, rows), :], hsem.at[p, k]
        )
        hcopy.start()
        pieces.append((k, p, at, rows, hcopy))
    pl.semaphore_wait(bar, 10)
    sends = []
    swaps = []
    for k, p, at, rows, hcopy in pieces:
        cp = rcopy(
            coarse_hbm.at[rows_at(other + at, rows), :], swap.at[rows_at(at, rows), :],
            s0.at[p, k], q0.at[p, k], partner,
        )
        cp.start()
        swaps.append(cp)
    loads = [
        pltpu.make_async_copy(src, dst, lsem.at[i])
        for i, (src, dst) in enumerate(
            ((w_hbm, w_ref), (x1_hbm, x1_ref), (res_hbm, res_ref))
        )
    ]
    pend = []
    sent1 = {}
    for (k, p, at, rows, hcopy), cp in zip(pieces, swaps):
        hcopy.wait()
        cp.wait_recv()
        add_into(acc, at, [(swap, at)], rows)
        if k:
            cp1 = rcopy(
                acc.at[rows_at(at, rows), :], r1.at[k - 1, pl.ds(BASE[p] // 4, rows), :],
                s1.at[p, k - 1], q1.at[p, k - 1], along(order[p][0], k),
            )
            sent1[p, k] = cp1
            pend.append(cp1)
        if len(pend) > 1:
            pend.pop(0).start()
    for cp1 in pend:
        cp1.start()
    for cp in loads:
        cp.start()
    find_hubs(cnt_ref, hub_ref, rank_ref)
    id_refs = (id0, id1, id2, id3)

    def fetch(src, n, g):
        part = src.at[pl.ds(pl.multiple_of(n * GROUP * BS, GROUP * BS), GROUP * BS)]
        return pltpu.make_async_copy(part, id_refs[g], isem.at[g])

    for g in range(2):
        fetch(agg_hbm, g, g).start()
        fetch(ids_hbm, g + 2, g + 2).start()
    cur = []
    sent2 = {}
    for p in PACE:
        rows = UNIT[p] * 16
        at = BASE[p] + xyz[order[p][0]] * rows
        for k in range(1, 4):
            sent1[p, k].wait_recv()
        add_into(acc, at, [(r1.at[k], BASE[p] // 4) for k in range(3)], rows)
        n2 = UNIT[p] * 4
        for k in range(1, 4):
            a = lax.rem(xyz[order[p][1]] + k, 4)
            sent2[p, k] = rcopy(
                acc.at[rows_at(at + a * n2, n2), :], r2.at[k - 1, pl.ds(BASE[p] // 16, n2), :],
                s2.at[p, k - 1], q2.at[p, k - 1], along(order[p][1], k),
            )
            sent2[p, k].start()
        cur.append((p, at + xyz[order[p][1]] * n2))
    sent3 = {}
    last = []
    for p, at in cur:
        rows = UNIT[p] * 4
        for k in range(1, 4):
            sent2[p, k].wait_recv()
        add_into(acc, at, [(r2.at[k], BASE[p] // 16) for k in range(3)], rows)
        n3 = UNIT[p]
        for k in range(1, 4):
            a = lax.rem(xyz[order[p][2]] + k, 4)
            sent3[p, k] = rcopy(
                acc.at[rows_at(at + a * n3, n3), :], r3.at[k - 1, pl.ds(BASE[p] // 64, n3), :],
                s3.at[p, k - 1], q3.at[p, k - 1], along(order[p][2], k),
            )
            sent3[p, k].start()
        last.append((p, at + xyz[order[p][2]] * n3))

    def spread(sent, p, dim, at, rows, ssem, rsem):
        for k in range(1, 4):
            ref = corr.at[rows_at(half + at, rows), :]
            cp = rcopy(ref, ref, ssem.at[p, k - 1], rsem.at[p, k - 1], along(dim, k))
            cp.start()
            sent[p, k] = cp
            sends.append(cp)

    def widen(at, rows):
        def go(i, _):
            here = rows_at(at + i * 16, 16)
            cf[here, :] = corr[here, :].astype(f32)
            return 0

        lax.fori_loop(0, rows // 16, go, 0)

    g3, g2, g1 = {}, {}, {}
    for p, at in last:
        rows = UNIT[p]
        for k in range(1, 4):
            sent3[p, k].wait_recv()
        for i in range(rows // 16):
            v = acc[rows_at(at + i * 16, 16), :]
            for k in range(3):
                v = v + r3[k, pl.ds(BASE[p] // 64 + i * 16, 16), :]
            div = jnp.concatenate(
                [jnp.full((1, BS), diag_ref[half + at + i * 16 + r], f32) for r in range(16)], axis=0
            )
            corr[rows_at(half + at + i * 16, 16), :] = (v / div).astype(bf16)
        spread(g3, p, order[p][2], at, rows, a3s, a3r)
    cur = []
    for p, at in last:
        for k in range(1, 4):
            g3[p, k].wait_recv()
        at = at - xyz[order[p][2]] * UNIT[p]
        cur.append((p, at))
        spread(g2, p, order[p][1], at, UNIT[p] * 4, a2s, a2r)
    swapped = []

    def hand_over(p, a, k):
        rows = UNIT[p] * 16
        ref = corr.at[rows_at(half + BASE[p] + a * rows, rows), :]
        cp = rcopy(ref, ref, cs.at[p, k], cr.at[p, k], partner)
        cp.start()
        sends.append(cp)
        swapped.append((cp, other + BASE[p] + a * rows, rows))
        widen(half + BASE[p] + a * rows, rows)

    for p, at in cur:
        for k in range(1, 4):
            g2[p, k].wait_recv()
        at = at - xyz[order[p][1]] * UNIT[p] * 4
        spread(g1, p, order[p][0], at, UNIT[p] * 16, a1s, a1r)
        hand_over(p, xyz[order[p][0]], 0)
    for k, p in [(k, p) for g in range(0, PARTS, 3) for k in (1, 3, 2) for p in PACE[g : g + 3]]:
        g1[p, k].wait_recv()
        hand_over(p, lax.rem(xyz[order[p][0]] + 4 - k, 4), k)
    for cp, at, rows in swapped:
        cp.wait_recv()
        widen(at, rows)
    for cp in loads:
        cp.wait()

    def local(i, _):
        for g in range(2):
            n = 2 * i + g
            fetch(agg_hbm, n, g).wait()
            for u in range(GROUP):
                b = n * GROUP + u
                for r in range(BS):
                    pcl[b, pl.ds(r, 1), :] = cf[pl.ds(id_refs[g][u * BS + r], 1), :]
                if u:
                    table[b - 1] = pcl[b - 1].astype(bf16)
            table[b] = pcl[b].astype(bf16)

            @pl.when(i == 0)
            def _():
                fetch(agg_hbm, n + 2, g).start()

        return 0

    lax.fori_loop(0, 2, local, 0)
    for g in range(2):
        fetch(ids_hbm, g, g).start()
    tiles = (tile0, tile1)

    def remote(i, _):
        for g in range(4):
            n = 4 * i + g
            fetch(ids_hbm, n, g).wait()
            for u in range(GROUP):
                t = NB + n * GROUP + u
                tile = tiles[u % 2]
                for r in range(BS):
                    tile[pl.ds(r, 1), :] = cf[pl.ds(id_refs[g][u * BS + r], 1), :]
                if u:
                    table[t - 1] = tiles[(u - 1) % 2][...].astype(bf16)
            table[t] = tile[...].astype(bf16)

            @pl.when(i < 2 * ND // GROUP // 4 - 1)
            def _():
                fetch(ids_hbm, n + 4, g).start()

        return 0

    lax.fori_loop(0, 2 * ND // GROUP // 4, remote, 0)

    def third(b, off):
        deg = column_of(deg_ref[b])
        pc = pcl[b]
        out_ref[b] = (x1_ref[b] + pc) + damping * (res_ref[b] - (deg * pc - off)) / deg

    stencil(w_ref, table, col_ref, cnt_ref, hub_ref, rank_ref, hacc, third)
    for cp in list(sent1.values()) + list(sent2.values()) + list(sent3.values()) + swaps + sends:
        cp.wait_send()


def coarse_leg(columns, counts, diag, degree, agg, ids, coarse, x1, res, weights):
    vm = pl.BlockSpec(memory_space=VMEM)
    sm = pl.BlockSpec(memory_space=SMEM)
    hbm = pl.BlockSpec(memory_space=pltpu.HBM)
    dma = pltpu.SemaphoreType.DMA
    return pl.pallas_call(
        coarse_kernel,
        out_shape=VMEM((NB, BS, BS), f32),
        in_specs=[sm, sm, sm, vm, hbm, hbm, hbm, hbm, hbm, hbm],
        out_specs=vm,
        scratch_shapes=[
            VMEM((NB, 16, BS, BS), bf16),
            VMEM((NB, BS, BS), f32),
            VMEM((NB, BS, BS), f32),
            SMEM((GROUP * BS,), jnp.int32),
            SMEM((GROUP * BS,), jnp.int32),
            SMEM((GROUP * BS,), jnp.int32),
            SMEM((GROUP * BS,), jnp.int32),
            VMEM((HALF, BS), f32),
            VMEM((HALF, BS), f32),
            VMEM((3, HALF // 4, BS), f32),
            VMEM((3, HALF // 16, BS), f32),
            VMEM((3, HALF // 64, BS), f32),
            VMEM((NC, BS), bf16),
            VMEM((NC, BS), f32),
            VMEM((TB, BS, BS), bf16),
            VMEM((NB, BS, BS), f32),
            VMEM((BS, BS), f32),
            VMEM((BS, BS), f32),
            VMEM((HUBS, BS, BS), f32),
            SMEM((HUBS,), jnp.int32),
            SMEM((NB,), jnp.int32),
            dma((3,)), dma((4,)),
            dma((PARTS, 4)), dma((PARTS, 4)), dma((PARTS, 4)),
            dma((PARTS, 3)), dma((PARTS, 3)), dma((PARTS, 3)), dma((PARTS, 3)), dma((PARTS, 3)), dma((PARTS, 3)),
            dma((PARTS, 3)), dma((PARTS, 3)), dma((PARTS, 3)), dma((PARTS, 3)), dma((PARTS, 3)), dma((PARTS, 3)),
            dma((PARTS, 4)), dma((PARTS, 4)),
        ],
        compiler_params=pltpu.CompilerParams(
            collective_id=1, has_side_effects=True, vmem_limit_bytes=60 * 2**20
        ),
        name="coarse_leg",
    )(columns, counts, diag, degree, agg, ids, coarse, x1, res, weights)


def body(rhs, guess, degree, weights, columns, block_counts, send_lists, aggregates, coarse_diag):
    cols = columns.T
    lists = send_lists[0].T
    deg = degree.reshape(NB, 1, BS)
    x1, res, ids = halo(
        cols, block_counts, lists,
        guess.reshape(NB, BS, BS), rhs.reshape(NB, BS, BS), deg,
        aggregates.reshape(NB, 1, BS), weights,
    )
    coarse = scatter(aggregates, res.reshape(NB * BS, BS))
    out = coarse_leg(
        cols, block_counts, coarse_diag, deg, aggregates, ids.reshape(-1), coarse, x1, res, weights
    )
    return out.reshape(NB * BS, BS)


def solution(mesh):
    both = ("rows", "cores")
    return jax.shard_map(
        body,
        mesh=mesh,
        in_specs=(
            P(both, None),
            P(both, None),
            P(both),
            P(both, None, None, None),
            P(both, None),
            P(both),
            P(both, None, None),
            P(both),
            P(),
        ),
        out_specs=P(both, None),
        check_vma=False,
    )
```
